32 devices in a mesh: gx: 4 (over z), gy: 2 (over y), gz: 4 (over x, core).
Axes of the slice: x: 2, y: 2, z: 4, core: 2. Of those that a mesh axis runs over, the one named last changes fastest.
Arguments:
- displacement: float32 [3, 64, 64, 1024], P(None, 'gx', 'gy', 'gz'), may hold values from -1.5 to 1.5
- density: float32 [64, 64, 1024], P('gx', 'gy', 'gz'), may hold values from 0.03 to 1
- stiffness: float32 [24, 24], replicated, may hold values from -9 to 9.5, as said below
Outputs:
- filtered: float32 [64, 64, 1024], P('gx', 'gy', 'gz')
- compliance: float32 [], replicated
- volume: float32 [], replicated
The draws below stay inside these ranges and needn't reach their ends.
Inputs may be any that keep to these rules, and one draw needn't show every extreme that they name: `stiffness`: symmetric and positive definite, every eigenvalue at least 0.5.
All inputs are finite; a program needn't handle non-finite values.
Results may differ from the reference program's by a relative error of at most 0.00005.
Values sent between devices are 32-bit elements; how exact they have to be, the bound alone decides.
A program may use at most 64 MiB of HBM per device.

```python
import jax
import jax.numpy as jnp
from jax import lax

NX = 64
NY = 64
NZ = 1024


def draw_density(key, part):
    levels = jax.random.uniform(key, (NX, NY, NZ), jnp.float32, 0.1, 1.0)
    rising = (1.0 + 2.0 * jnp.arange(NX, dtype=jnp.float32) / max(NX - 1, 1)) / 3.0
    return levels * rising[:, None, None]


def draw_stiffness(key, part):
    factors = jax.random.truncated_normal(key, -3.0, 3.0, (24, 24), jnp.float32)
    factors = factors / jnp.sqrt(24.0)
    return jnp.dot(factors, factors.T, precision=lax.Precision.HIGHEST) + 0.5 * jnp.eye(24, dtype=jnp.float32)


def level_of(own_key, dims, cuts, least, top_value):
    def one(axis_at, shards_of):
        steps = jax.random.uniform(jax.random.fold_in(jax.random.fold_in(own_key, 6), axis_at), (shards_of,), jnp.float32, least / len(cuts), top_value / len(cuts))
        return jnp.repeat(jnp.exp(steps), dims[axis_at] // shards_of).reshape((-1,) + (1,) * (len(dims) - axis_at - 1))

    level = one(*cuts[0])
    for cut in cuts[1:]:
        level = level * one(*cut)
    return level


def bell_draw(key, dims, deviation, bound, pieces=(), kind=jnp.bfloat16):
    values = deviation * jax.random.normal(key, dims, jnp.float32)
    if pieces:
        values = values * level_of(key, dims, pieces, -0.22, 0.18)
    return jnp.clip(values, -bound, bound).astype(kind)


def setup_inputs(seed: int = 0) -> dict:
    seeds = jax.random.split(jax.random.key(seed), 4)
    displacement = bell_draw(seeds[0], (3, NX, NY, NZ), 0.25, 1.5, ((1, 4), (2, 2), (3, 4)), jnp.float32)
    density = draw_density(jax.random.fold_in(seeds[3], 71), 0)
    stiffness = draw_stiffness(jax.random.fold_in(seeds[3], 71), 0)
    return {"displacement": displacement, "density": density, "stiffness": stiffness}


VOID_STIFFNESS = 1e-3
KERNEL = (1.0, 2.0, 3.0, 2.0, 1.0)


def smooth(values, along):
    length = values.shape[along] - 4
    summed = None
    for offset in range(5):
        section = lax.slice_in_dim(values, offset, offset + length, axis=along)
        scaled = KERNEL[offset] * section
        summed = scaled if summed is None else summed + scaled
    return summed


def side_sums(first, amount, extent):
    position = first + jnp.arange(amount, dtype=jnp.int32)
    summed = jnp.zeros((amount,), jnp.float32)
    for offset in range(5):
        inside = (position + offset - 2 >= 0) & (position + offset - 2 < extent)
        summed = summed + KERNEL[offset] * inside.astype(jnp.float32)
    return summed


def plane_energy(slab_nodes, stiffness):
    height = slab_nodes.shape[2] - 1
    length = slab_nodes.shape[3] - 1
    corner_rows = jnp.stack([slab_nodes[member, along_x, along_y:along_y + height, along_z:along_z + length].reshape(-1)
                             for member in range(3) for along_x in range(2) for along_y in range(2) for along_z in range(2)])
    product = jnp.dot(stiffness, corner_rows, precision=lax.Precision.HIGHEST, preferred_element_type=jnp.float32)
    return jnp.sum(corner_rows * product, axis=0).reshape(height, length)


def energies(node_field, stiffness, planes):
    def one_plane(plane_index):
        slab_nodes = lax.dynamic_slice_in_dim(node_field, plane_index, 2, 1)
        return plane_energy(slab_nodes, stiffness)
    return lax.map(one_plane, jnp.arange(planes, dtype=jnp.int32))


def reference(displacement, density, stiffness):
    node_field = jnp.pad(displacement, ((0, 0), (0, 1), (0, 1), (0, 1)))
    energy = energies(node_field, stiffness, NX)
    modulus = VOID_STIFFNESS + density * density * density * (1.0 - VOID_STIFFNESS)
    cell_count = float(NX * NY * NZ)
    compliance = jnp.sum(modulus * energy) / cell_count
    volume = jnp.sum(density) / cell_count
    sensitivity = -3.0 * (1.0 - VOID_STIFFNESS) * density * density * energy
    hole_sum = side_sums(0, NX, NX)[:, None, None] * side_sums(0, NY, NY)[None, :, None] * side_sums(0, NZ, NZ)[None, None, :]
    weighted = sensitivity / hole_sum
    padded = jnp.pad(weighted, 2)
    filtered = smooth(smooth(smooth(padded, 0), 1), 2)
    return filtered, compliance, volume
```

```python
import functools

import jax
import jax.numpy as jnp
from jax import lax
from jax.experimental import pallas as pl
from jax.experimental.pallas import tpu as pltpu
from jax.sharding import PartitionSpec as P

VOID = 0.001
H = (1.0, 2.0, 3.0, 2.0, 1.0)
MESH = pl.DeviceIdType.MESH
AXES = ("gx", "gy", "gz")
F32 = jnp.float32
BF16 = jnp.bfloat16
NODE_STEPS = [(a, b, c) for a in (0, 1) for b in (0, 1) for c in (0, 1) if a + b + c]
SIDE_STEPS = [(b, c) for b in (-1, 0, 1) for c in (-1, 0, 1) if b or c]


def iota(shape, dim):
    return lax.broadcasted_iota(jnp.int32, shape, dim)


def line_sum(position, extent):
    total = None
    for d in range(5):
        at = position + (d - 2)
        term = jnp.where((at >= 0) & (at < extent), H[d], 0.0).astype(F32)
        total = term if total is None else total + term
    return total


def band_weights(stiff):
    rows, cols = 192, 128
    pick = jnp.where((iota((rows, 24), 0) >> 3) == iota((rows, 24), 1), 1.0, 0.0).astype(F32)

    def column(shape):
        col = iota(shape, 1)
        a, m, s = col >> 6, (col >> 4) & 3, col & 15
        edge = m == 3
        c = jnp.where(edge, jnp.where(s >= 3, 1, 0), s >> 3)
        m = jnp.where(edge, s - 3 * c, m)
        valid = jnp.logical_not(edge) | (s < 6)
        return 8 * m + 4 * a + c, valid, jnp.where(edge, 8, s & 7)

    total = None
    for b in (0, 1):
        q, valid, _ = column((24, cols))
        place = jnp.where((iota((24, cols), 0) == q + 2 * b) & valid, 1.0, 0.0).astype(F32)
        wide = jnp.dot(stiff, place, precision=lax.Precision.HIGHEST, preferred_element_type=F32)
        tall = jnp.dot(pick, wide, precision=lax.Precision.HIGHEST, preferred_element_type=F32)
        _, _, jj = column((rows, cols))
        term = jnp.where(jj - (iota((rows, cols), 0) & 7) == b, tall, 0.0)
        total = term if total is None else total + term
    high = total.astype(BF16)
    return jnp.concatenate([high, (total - high.astype(F32)).astype(BF16)], 1)


def kernel(
    sizes, u_hbm, rho_hbm, stiff_hbm, out, packs, totals,
    u, rho, stiff, rx, ry, rxy, rz, ys, yd, zs, field, edge, line_f, line_u, parts, weights, wx, wy,
    yslo, yshi, rylo, ryhi, zslo, zshi, rzz, sums, insem, nsend, nrecv, fsend, frecv, gsend, grecv,
):
    ni, nj, nk = rho.shape
    n = dict(zip(AXES, sizes))
    me = {axis: lax.axis_index(axis) for axis in AXES}
    ny, nz = n["gy"], n["gz"]
    down = {axis: me[axis] > 0 for axis in AXES}
    up = {axis: me[axis] < n[axis] - 1 for axis in AXES}

    loads = []
    for at, (src, dst) in enumerate(((stiff_hbm, stiff), (u_hbm, u), (rho_hbm, rho))):
        copy = pltpu.make_async_copy(src, dst, insem.at[at])
        copy.start()
        loads.append(copy)

    def hop(step):
        ids, ok = {}, None
        for axis, s in zip(AXES, step):
            if s:
                ids[axis] = me[axis] + s
                flag = up[axis] if s > 0 else down[axis]
                ok = flag if ok is None else jnp.logical_and(ok, flag)
        return ids, ok

    def minus(step):
        return tuple(-s for s in step)

    line = [{"gx": lax.rem(me["gx"] + off, n["gx"])} for off in range(1, n["gx"])]
    sheet = [
        {"gy": lax.rem(me["gy"] + off // nz, ny), "gz": lax.rem(me["gz"] + off % nz, nz)}
        for off in range(1, ny * nz)
    ]
    barrier = pltpu.get_barrier_semaphore()
    for ids in line + sheet:
        pl.semaphore_signal(barrier, inc=1, device_id=ids, device_id_type=MESH)
    peers = len(line) + len(sheet)
    for step in NODE_STEPS:
        if step[0] and sum(step) > 1:
            for way in (step, minus(step)):
                ids, ok = hop(way)
                peers = peers + jnp.where(ok, 1, 0)

                @pl.when(ok)
                def _():
                    pl.semaphore_signal(barrier, inc=1, device_id=ids, device_id_type=MESH)

    pl.semaphore_wait(barrier, peers)

    def swap(copies, src, dst, send_sem, recv_sem, step):
        ids, sends = hop(step)
        copy = pltpu.make_async_remote_copy(
            src_ref=src, dst_ref=dst, send_sem=send_sem, recv_sem=recv_sem,
            device_id=ids, device_id_type=MESH,
        )
        copies.append((copy, sends, hop(minus(step))[1], dst))

        @pl.when(sends)
        def _():
            copy.start()

    def arrive(copies):
        for copy, _, takes, dst in copies:

            @pl.when(takes)
            def _():
                copy.wait_recv()

            @pl.when(jnp.logical_not(takes))
            def _():
                dst[...] = jnp.zeros(dst.shape, F32)

    def finish(copies):
        for copy, sends, _, _ in copies:

            @pl.when(sends)
            def _():
                copy.wait_send()

    beside, below, far = [], [], []

    def node_swap(step):
        a, b, c = step
        at = NODE_STEPS.index(step)
        if c:
            src, dst = (zs.at[0:8], rz.at[a, b, 0:8]) if b else (zs, rz.at[a, b])
        elif b:
            src, dst = (yd, rxy) if a else (ys, ry)
        else:
            src, dst = u_hbm.at[:, 0], rx
        copies = far if a else (below if b else beside)
        swap(copies, src, dst, nsend.at[at], nrecv.at[at], minus(step))

    node_swap((1, 0, 0))
    loads[1].wait()
    lane = iota((nj, 128), 1)
    packed = jnp.zeros((nj, 128), F32)
    for at in range(3 * ni):
        column = u[at // ni, at % ni, :, 0:128]
        packed = jnp.where(lane == at, pltpu.roll(column, at, 1) if at else column, packed)
    zs[...] = packed
    for step in NODE_STEPS:
        if step[2]:
            node_swap(step)
    yd[...] = jnp.zeros(yd.shape, F32)
    for m in range(3):
        for i in range(ni):
            ys[m, i : i + 1, :] = u[m, i, 0:1, :]
        yd[m : m + 1, :] = u[m, 0, 0:1, :]
    node_swap((0, 1, 0))
    node_swap((1, 1, 0))
    loads[0].wait()
    weights[...] = band_weights(stiff[...])

    last = iota((nj, nk), 1) == nk - 1
    last1 = iota((1, nk), 1) == nk - 1
    edge[...] = jnp.zeros(edge.shape, F32)

    def beyond(base, col, at, rim):
        side = pltpu.roll(col, 127 - at, 1)
        return jnp.where(rim, jnp.concatenate([side, side], 1), pltpu.roll(base, nk - 1, 1))

    def sharp(x):
        return x + (x - x.astype(BF16).astype(F32))

    def layer(m, to, base, moved):
        for c, x in enumerate((base, moved)):
            f = sharp(x)
            for h in range(2):
                field[c, m, to, h, 0:nj, :] = f[:, 128 * h : 128 * h + 128]
            for jt in range(1, nj // 8):
                edge[to, jt - 1, 3 * c + m : 3 * c + m + 1, :] = x[8 * jt : 8 * jt + 1, :]
        for jt in range(nj // 8):
            rows = slice(8 * jt, 8 * jt + 8)
            parts[jt, to, 16 * m : 16 * m + 16, :] = jnp.concatenate([base[rows], moved[rows]], 0).astype(BF16)

    def next_row(c, m, to, x, f):
        for h in range(2):
            field[c, m, to, h, nj : nj + 1, :] = f[:, 128 * h : 128 * h + 128]
        edge[to, nj // 8 - 1, 3 * c + m : 3 * c + m + 1, :] = x

    def own_layer(i, carry):
        for m in range(3):
            base = u[m, i]
            layer(m, i, base, beyond(base, rz[0, 0], m * ni + i, last))
        return carry

    def own_row(i, carry):
        for c in range(2):
            for m in range(3):
                at = pl.ds(i, 1)
                next_row(c, m, i, line_u[3 * c + m, at, :], line_f[3 * c + m, at, :])
        return carry

    loads[2].wait()
    wy[0, 0:nj, :] = 1.0 / (
        line_sum(me["gy"] * nj + iota((nj, nk), 0), ny * nj)
        * line_sum(me["gz"] * nk + iota((nj, nk), 1), nz * nk)
    )
    arrive(beside)
    lax.fori_loop(0, ni, own_layer, 0, unroll=2)
    arrive(below)
    for m in range(3):
        base = ry[m]
        mine = iota((ni, 128), 1) == iota((ni, 128), 0) + m * ni
        corner = jnp.sum(jnp.where(mine, rz[0, 1, 0:1, :], 0.0), axis=1, keepdims=True)
        moved = jnp.where(iota((ni, nk), 1) == nk - 1, corner, pltpu.roll(base, nk - 1, 1))
        for c, x in enumerate((base, moved)):
            line_u[3 * c + m] = x
            line_f[3 * c + m] = sharp(x)
    lax.fori_loop(0, ni, own_row, 0, unroll=4)
    arrive(far)
    for m in range(3):
        base = rx[m]
        layer(m, ni, base, beyond(base, rz[1, 0], m * ni, last))
        row = rxy[m : m + 1, :]
        moved = beyond(row, rz[1, 1, 0:1, :], m * ni, last1)
        for c, x in enumerate((row, moved)):
            next_row(c, m, ni, x, sharp(x))

    none8 = jnp.zeros((8, nk), F32)

    def tile(jt, p):
        return [parts[jt, p], jnp.concatenate([edge[p, jt], none8], 0).astype(BF16)]

    def plane(i, carry):
        c_sum, v_sum = carry
        inv_x = 1.0 / line_sum(jnp.full((8, nk), me["gx"] * ni + i, jnp.int32), n["gx"] * ni)
        for jt in range(nj // 8):
            data = tile(jt, i) + tile(jt, i + 1)
            product = jnp.dot(weights[...], jnp.concatenate(data + data, 0), preferred_element_type=F32)
            energy = None
            for r in range(24):
                m, a, b, c = r >> 3, (r >> 2) & 1, (r >> 1) & 1, r & 1
                rows = pl.ds(8 * jt + b, 8)
                f = [field[c, m, i + a, h, rows, :] for h in range(2)]
                term = product[8 * r : 8 * r + 8] * jnp.concatenate(f, 1)
                energy = term if energy is None else energy + term
            d = rho[i, 8 * jt : 8 * jt + 8, :]
            c_sum = c_sum + (VOID + d * d * d * (1.0 - VOID)) * energy
            v_sum = v_sum + d
            wx[i + 2, 8 * jt : 8 * jt + 8, :] = (
                (-3.0 * (1.0 - VOID)) * d * d * energy * (inv_x * wy[0, 8 * jt : 8 * jt + 8, :])
            )
        return c_sum, v_sum

    zero = jnp.zeros((8, nk), F32)
    carry = lax.fori_loop(
        0, 4, lambda t, s: plane(jnp.where(t < 2, t, ni - 4 + t), s), (zero, zero)
    )
    x_copies = []
    swap(x_copies, wx.at[2:4], wx.at[ni + 2 : ni + 4], fsend.at[8], frecv.at[8], (-1, 0, 0))
    swap(x_copies, wx.at[ni : ni + 2], wx.at[0:2], fsend.at[9], frecv.at[9], (1, 0, 0))
    c_sum, v_sum = lax.fori_loop(4, ni, lambda t, s: plane(t - 2, s), carry)

    def share(base, mine, value, group):
        sums[base + mine] = value
        copies = []
        for off, ids in enumerate(group):
            copy = pltpu.make_async_remote_copy(
                src_ref=sums.at[base + mine], dst_ref=sums.at[base + mine],
                send_sem=gsend.at[base + off], recv_sem=grecv.at[base + off],
                device_id=ids, device_id_type=MESH,
            )
            copy.start()
            copies.append(copy)
        return copies

    def gather(base, copies):
        for copy in copies:
            copy.wait()
        total = sums[base]
        for at in range(1, len(copies) + 1):
            total = total + sums[base + at]
        return total


    def fold(x):
        row = jnp.sum(x, axis=0, keepdims=True)
        row = row[:, :128] + row[:, 128:]
        return row + pltpu.roll(row, 64, 1)

    partial = jnp.where(iota((1, 128), 1) < 64, fold(c_sum), fold(v_sum))
    x_sums = share(0, me["gx"], partial, line)
    arrive(x_copies)

    def smooth_x(i, carry):
        lo, hi = carry
        s = 3.0 * wx[i + 2] + 2.0 * (wx[i + 1] + wx[i + 3]) + (wx[i] + wx[i + 4])
        wy[i, 8 : 8 + nj, :] = s
        for at in range(2):
            yslo[at, pl.ds(i, 1), :] = s[at : at + 1]
            yshi[at, pl.ds(i, 1), :] = s[nj - 2 + at : nj - 1 + at]
        mine = (lane >> 1) == i
        lo = jnp.where(mine, pltpu.roll(s[:, 0:128], 2 * i, 1), lo)
        hi = jnp.where(mine, pltpu.roll(s[:, nk - 128 : nk], lax.rem(2 * i + 2, 128), 1), hi)
        return lo, hi

    none = jnp.zeros((nj, 128), F32)
    lo, hi = lax.fori_loop(0, ni, smooth_x, (none, none), unroll=4)
    zslo[...] = lo
    zshi[...] = hi
    side_copies = []
    for at, (b, c) in enumerate(SIDE_STEPS):
        if c:
            rows = (slice(nj - 8, nj), slice(0, nj), slice(0, 8))[1 - b]
            to = (slice(0, 8), slice(8, 8 + nj), slice(8 + nj, 16 + nj))[1 - b]
            src = (zslo if c < 0 else zshi).at[rows]
            dst = rzz.at[1 if c < 0 else 0, to]
        else:
            src, dst = (yslo, ryhi) if b < 0 else (yshi, rylo)
        swap(side_copies, src, dst, fsend.at[at], frecv.at[at], (0, b, c))
    all_sums = share(n["gx"], me["gy"] * nz + me["gz"], gather(0, x_sums), sheet)
    arrive(side_copies)

    def smooth_rows(ref, at):
        return (
            3.0 * ref[at, 8 : 8 + nj, :]
            + 2.0 * (ref[at, 7 : 7 + nj, :] + ref[at, 9 : 9 + nj, :])
            + (ref[at, 6 : 6 + nj, :] + ref[at, 10 : 10 + nj, :])
        )

    for side in range(2):
        packs[side] = smooth_rows(rzz, side)

    def smooth_y(i, carry):
        for at in range(2):
            wy[i, 6 + at : 7 + at, :] = rylo[at, pl.ds(i, 1), :]
            wy[i, 8 + nj + at : 9 + nj + at, :] = ryhi[at, pl.ds(i, 1), :]
        out[i] = smooth_rows(wy, i)
        return carry

    lax.fori_loop(0, ni, smooth_y, 0, unroll=4)
    totals[...] = gather(n["gx"], all_sums)
    for copies in (beside, below, far, x_copies, side_copies):
        finish(copies)


def last_pass(cells, field, packs, totals, out, comp, vol):
    ni, nj, nk = field.shape
    both = totals[...]
    first = iota((1, 128), 1) < 64
    comp[0, 0] = jnp.sum(jnp.where(first, both, 0.0)) / cells
    vol[0, 0] = jnp.sum(jnp.where(first, 0.0, both)) / cells
    lanes = iota((nj, nk), 1)
    even = lax.rem(iota((nj, 128), 1), 2) == 0
    left, right = packs[0], packs[1]
    left = jnp.where(even, left + 2.0 * pltpu.roll(left, 127, 1), left)
    right = jnp.where(even, right, right + 2.0 * pltpu.roll(right, 1, 1))
    apart = jnp.abs(iota((nk, nk), 0) - iota((nk, nk), 1))
    band = jnp.maximum(3 - apart, 0).astype(F32).astype(BF16)

    def twice(x):
        return jnp.concatenate([x, x], 1)

    for i in range(ni):
        t = field[i]
        high = t.astype(BF16)
        low = (t - high.astype(F32)).astype(BF16)
        own = jnp.dot(high, band, preferred_element_type=F32) + jnp.dot(low, band, preferred_element_type=F32)
        lo = twice(pltpu.roll(left, (128 - 2 * i) % 128, 1))
        hi = twice(pltpu.roll(right, 126 - 2 * i, 1))
        out[i] = own + jnp.where(lanes < 2, lo, jnp.where(lanes >= nk - 2, hi, 0.0))


def on_device(sizes, displacement, density, stiffness):
    ni, nj, nk = density.shape
    vmem = pl.BlockSpec(memory_space=pltpu.VMEM)
    smem = pl.BlockSpec(memory_space=pltpu.SMEM)
    hbm = pl.BlockSpec(memory_space=pltpu.HBM)
    members = sizes[0] + sizes[1] * sizes[2]
    scratch = [
        displacement.shape, density.shape, stiffness.shape,
        (3, nj, nk), (3, ni, nk), (8, nk), (2, 2, nj, 128), (3, ni, nk), (8, nk), (nj, 128),
        (2, 3, ni + 1, 2, nj + 8, 128), (ni + 1, nj // 8, 8, nk), (6, ni, nk), (6, ni, nk),
    ]
    later = [
        (ni + 4, nj, nk), (ni, nj + 16, nk),
        (2, ni, nk), (2, ni, nk), (2, ni, nk), (2, ni, nk),
        (nj, 128), (nj, 128), (2, nj + 16, 128), (members, 1, 128),
    ]
    field, packs, totals = pl.pallas_call(
        functools.partial(kernel, sizes),
        out_shape=(
            jax.ShapeDtypeStruct((ni, nj, nk), F32),
            jax.ShapeDtypeStruct((2, nj, 128), F32),
            jax.ShapeDtypeStruct((1, 128), F32),
        ),
        in_specs=[hbm] * 3,
        out_specs=(vmem, vmem, vmem),
        scratch_shapes=[pltpu.VMEM(shape, F32) for shape in scratch]
        + [pltpu.VMEM((nj // 8, ni + 1, 48, nk), BF16), pltpu.VMEM((192, 256), BF16)]
        + [pltpu.VMEM(shape, F32) for shape in later]
        + [pltpu.SemaphoreType.DMA((count,)) for count in (3, 7, 7, 10, 10, members, members)],
        compiler_params=pltpu.CompilerParams(
            collective_id=0, has_side_effects=True, vmem_limit_bytes=24 * 1024 * 1024
        ),
    )(*(pltpu.with_memory_space_constraint(x, pltpu.HBM) for x in (displacement, density, stiffness)))
    cells = float(ni * nj * nk * sizes[0] * sizes[1] * sizes[2])
    filtered, comp, vol = pl.pallas_call(
        functools.partial(last_pass, cells),
        out_shape=(
            jax.ShapeDtypeStruct((ni, nj, nk), F32),
            jax.ShapeDtypeStruct((1, 1), F32),
            jax.ShapeDtypeStruct((1, 1), F32),
        ),
        in_specs=[vmem] * 3,
        out_specs=(vmem, smem, smem),
        compiler_params=pltpu.CompilerParams(vmem_limit_bytes=24 * 1024 * 1024),
    )(field, packs, totals)
    return filtered, comp.reshape(()), vol.reshape(())


def solution(mesh):
    sizes = tuple(mesh.shape[axis] for axis in AXES)
    return jax.shard_map(
        functools.partial(on_device, sizes),
        mesh=mesh,
        in_specs=(P(None, "gx", "gy", "gz"), P("gx", "gy", "gz"), P()),
        out_specs=(P("gx", "gy", "gz"), P(), P()),
        check_vma=False,
    )
```

```python
import functools

import jax
import jax.numpy as jnp
from jax import lax
from jax.experimental import pallas as pl
from jax.experimental.pallas import tpu as pltpu
from jax.sharding import PartitionSpec as P

VOID = 0.001
H = (1.0, 2.0, 3.0, 2.0, 1.0)
MESH = pl.DeviceIdType.MESH
AXES = ("gx", "gy", "gz")
F32 = jnp.float32
BF16 = jnp.bfloat16
NODE_STEPS = [(a, b, c) for a in (0, 1) for b in (0, 1) for c in (0, 1) if a + b + c]
SIDE_STEPS = [(b, c) for b in (-1, 0, 1) for c in (-1, 0, 1) if b or c]


def iota(shape, dim):
    return lax.broadcasted_iota(jnp.int32, shape, dim)


def line_sum(position, extent):
    total = None
    for d in range(5):
        at = position + (d - 2)
        term = jnp.where((at >= 0) & (at < extent), H[d], 0.0).astype(F32)
        total = term if total is None else total + term
    return total


def band_weights(stiff):
    rows, cols = 192, 128
    pick = jnp.where((iota((rows, 24), 0) >> 3) == iota((rows, 24), 1), 1.0, 0.0).astype(F32)

    def column(shape):
        col = iota(shape, 1)
        a, m, s = col >> 6, (col >> 4) & 3, col & 15
        edge = m == 3
        c = jnp.where(edge, jnp.where(s >= 3, 1, 0), s >> 3)
        m = jnp.where(edge, s - 3 * c, m)
        valid = jnp.logical_not(edge) | (s < 6)
        return 8 * m + 4 * a + c, valid, jnp.where(edge, 8, s & 7)

    total = None
    for b in (0, 1):
        q, valid, _ = column((24, cols))
        place = jnp.where((iota((24, cols), 0) == q + 2 * b) & valid, 1.0, 0.0).astype(F32)
        wide = jnp.dot(stiff, place, precision=lax.Precision.HIGHEST, preferred_element_type=F32)
        tall = jnp.dot(pick, wide, precision=lax.Precision.HIGHEST, preferred_element_type=F32)
        _, _, jj = column((rows, cols))
        term = jnp.where(jj - (iota((rows, cols), 0) & 7) == b, tall, 0.0)
        total = term if total is None else total + term
    high = total.astype(BF16)
    return jnp.concatenate([high, (total - high.astype(F32)).astype(BF16)], 1)


def kernel(
    sizes, u_hbm, rho_hbm, stiff_hbm, out, packs, totals,
    u, rho, stiff, rx, ry, rxy, rz, ys, yd, zs, field, edge, line_f, line_u, inv, parts, weights, wx, wy,
    yslo, yshi, rylo, ryhi, zslo, zshi, rzz, sums, insem, nsend, nrecv, fsend, frecv, gsend, grecv,
):
    ni, nj, nk = rho.shape
    n = dict(zip(AXES, sizes))
    me = {axis: lax.axis_index(axis) for axis in AXES}
    ny, nz = n["gy"], n["gz"]
    down = {axis: me[axis] > 0 for axis in AXES}
    up = {axis: me[axis] < n[axis] - 1 for axis in AXES}

    loads = []
    for at, (src, dst) in enumerate(((stiff_hbm, stiff), (u_hbm, u), (rho_hbm, rho))):
        copy = pltpu.make_async_copy(src, dst, insem.at[at])
        copy.start()
        loads.append(copy)

    def hop(step):
        ids, ok = {}, None
        for axis, s in zip(AXES, step):
            if s:
                ids[axis] = me[axis] + s
                flag = up[axis] if s > 0 else down[axis]
                ok = flag if ok is None else jnp.logical_and(ok, flag)
        return ids, ok

    def minus(step):
        return tuple(-s for s in step)

    line = [{"gx": lax.rem(me["gx"] + off, n["gx"])} for off in range(1, n["gx"])]
    sheet = [
        {"gy": lax.rem(me["gy"] + off // nz, ny), "gz": lax.rem(me["gz"] + off % nz, nz)}
        for off in range(1, ny * nz)
    ]
    barrier = pltpu.get_barrier_semaphore()
    for ids in line + sheet:
        pl.semaphore_signal(barrier, inc=1, device_id=ids, device_id_type=MESH)
    peers = len(line) + len(sheet)
    for step in NODE_STEPS:
        if step[0] and sum(step) > 1:
            for way in (step, minus(step)):
                ids, ok = hop(way)
                peers = peers + jnp.where(ok, 1, 0)

                @pl.when(ok)
                def _():
                    pl.semaphore_signal(barrier, inc=1, device_id=ids, device_id_type=MESH)

    pl.semaphore_wait(barrier, peers)

    def swap(copies, src, dst, send_sem, recv_sem, step):
        ids, sends = hop(step)
        copy = pltpu.make_async_remote_copy(
            src_ref=src, dst_ref=dst, send_sem=send_sem, recv_sem=recv_sem,
            device_id=ids, device_id_type=MESH,
        )
        copies.append((copy, sends, hop(minus(step))[1], dst))

        @pl.when(sends)
        def _():
            copy.start()

    def arrive(copies):
        for copy, _, takes, dst in copies:

            @pl.when(takes)
            def _():
                copy.wait_recv()

            @pl.when(jnp.logical_not(takes))
            def _():
                dst[...] = jnp.zeros(dst.shape, F32)

    def finish(copies):
        for copy, sends, _, _ in copies:

            @pl.when(sends)
            def _():
                copy.wait_send()

    beside, below, far = [], [], []

    def node_swap(step):
        a, b, c = step
        at = NODE_STEPS.index(step)
        if c:
            src, dst = (zs.at[0:8], rz.at[a, b, 0:8]) if b else (zs, rz.at[a, b])
        elif b:
            src, dst = (yd, rxy) if a else (ys, ry)
        else:
            src, dst = u_hbm.at[:, 0], rx
        copies = far if a else (below if b else beside)
        swap(copies, src, dst, nsend.at[at], nrecv.at[at], minus(step))

    node_swap((1, 0, 0))
    loads[1].wait()
    lane = iota((nj, 128), 1)
    packed = jnp.zeros((nj, 128), F32)
    for at in range(3 * ni):
        column = u[at // ni, at % ni, :, 0:128]
        packed = jnp.where(lane == at, pltpu.roll(column, at, 1) if at else column, packed)
    zs[...] = packed
    for step in NODE_STEPS:
        if step[2]:
            node_swap(step)
    yd[...] = jnp.zeros(yd.shape, F32)
    for m in range(3):
        for i in range(ni):
            ys[m, i : i + 1, :] = u[m, i, 0:1, :]
        yd[m : m + 1, :] = u[m, 0, 0:1, :]
    node_swap((0, 1, 0))
    node_swap((1, 1, 0))
    loads[0].wait()
    weights[...] = band_weights(stiff[...])

    last = iota((nj, 128), 1) == 127
    edge[...] = jnp.zeros(edge.shape, F32)
    nq = nj // 16

    def sharp(x):
        return x + (x - x.astype(BF16).astype(F32))

    def pair(x, q):
        return jnp.concatenate([x[16 * q : 16 * q + 8], x[16 * q + 8 : 16 * q + 16]], 1)

    def layer(h, to, at, source, col):
        for m in range(3):
            x = source(m, h)
            side = source(m, 1) if h == 0 else col
            turn = 127 if h == 0 else 127 - (m * ni + at)
            moved = jnp.where(last, pltpu.roll(side, turn, 1), pltpu.roll(x, 127, 1))
            for c, y in enumerate((x, moved)):
                field[c, m, to, h, 0:nj, :] = sharp(y)
                for jt in range(nj // 8 - 1):
                    edge[h, jt // 2, to, 3 * c + m : 3 * c + m + 1, 128 * (jt % 2) : 128 * (jt % 2) + 128] = (
                        y[8 * jt + 8 : 8 * jt + 9, :]
                    )
            for q in range(nq):
                parts[h, q, to, 16 * m : 16 * m + 16, :] = jnp.concatenate([pair(x, q), pair(moved, q)], 0).astype(BF16)

    def own(i):
        return lambda m, h: u[m, i, :, 128 * h : 128 * h + 128]

    def next_row(c, m, to, x, f):
        for h in range(2):
            half = slice(128 * h, 128 * h + 128)
            field[c, m, to, h, nj : nj + 1, :] = f[:, half]
            edge[h, nq - 1, to, 3 * c + m : 3 * c + m + 1, 128:256] = x[:, half]

    def own_row(i, carry):
        for c in range(2):
            for m in range(3):
                at = pl.ds(i, 1)
                next_row(c, m, i, line_u[3 * c + m, at, :], line_f[3 * c + m, at, :])
        return carry

    none8 = jnp.zeros((8, nk), F32)

    def tile(h, q, p):
        return [parts[h, q, p], jnp.concatenate([edge[h, q, p], none8], 0).astype(BF16)]

    def unit(i, q, h, c_sum, v_sum):
        half = slice(128 * h, 128 * h + 128)
        rows = [slice(16 * q + 8 * t, 16 * q + 8 * t + 8) for t in range(2)]
        data = tile(h, q, i) + tile(h, q, i + 1)
        product = jnp.dot(weights[...], jnp.concatenate(data + data, 0), preferred_element_type=F32)
        energy = None
        for r in range(24):
            m, a, b, c = r >> 3, (r >> 2) & 1, (r >> 1) & 1, r & 1
            f = [field[c, m, i + a, h, 16 * q + 8 * t + b : 16 * q + 8 * t + b + 8, :] for t in range(2)]
            term = product[8 * r : 8 * r + 8] * jnp.concatenate(f, 1)
            energy = term if energy is None else energy + term
        d = jnp.concatenate([rho[i, rows[t], half] for t in range(2)], 1)
        scale = jnp.concatenate([inv[rows[t], half] for t in range(2)], 1)
        inv_x = 1.0 / line_sum(jnp.full((8, nk), me["gx"] * ni + i, jnp.int32), n["gx"] * ni)
        w = (-3.0 * (1.0 - VOID)) * d * d * energy * (inv_x * scale)
        for t in range(2):
            wx[i + 2, rows[t], half] = w[:, 128 * t : 128 * t + 128]
        return c_sum + (VOID + d * d * d * (1.0 - VOID)) * energy, v_sum + d

    def sweep(h):
        def body(i, carry):
            layer(h, i + 1, i + 1, own(i + 1), rz[0, 0])
            return unit(i, 0, h, *carry)

        return body

    loads[2].wait()
    inv[...] = 1.0 / (
        line_sum(me["gy"] * nj + iota((nj, nk), 0), ny * nj)
        * line_sum(me["gz"] * nk + iota((nj, nk), 1), nz * nk)
    )
    carry = (none8, none8)
    layer(0, 0, 0, own(0), None)
    carry = lax.fori_loop(0, ni - 1, sweep(0), carry, unroll=5)
    arrive(beside)
    layer(1, 0, 0, own(0), rz[0, 0])
    carry = lax.fori_loop(0, ni - 1, sweep(1), carry, unroll=5)
    arrive(below)
    for m in range(3):
        base = ry[m]
        mine = iota((ni, 128), 1) == iota((ni, 128), 0) + m * ni
        corner = jnp.sum(jnp.where(mine, rz[0, 1, 0:1, :], 0.0), axis=1, keepdims=True)
        moved = jnp.where(iota((ni, nk), 1) == nk - 1, corner, pltpu.roll(base, nk - 1, 1))
        for c, x in enumerate((base, moved)):
            line_u[3 * c + m] = x
            line_f[3 * c + m] = sharp(x)
    lax.fori_loop(0, ni, own_row, 0, unroll=4)

    def upper(i, carry):
        for q in range(1, nq):
            for h in range(2):
                carry = unit(i, q, h, *carry)
        return carry

    carry = lax.fori_loop(0, ni - 1, upper, carry, unroll=5)
    x_copies = []
    swap(x_copies, wx.at[2:4], wx.at[ni + 2 : ni + 4], fsend.at[8], frecv.at[8], (-1, 0, 0))
    arrive(far)
    for h in range(2):
        layer(h, ni, 0, lambda m, h: rx[m, :, 128 * h : 128 * h + 128], rz[1, 0])
    for m in range(3):
        row = rxy[m : m + 1, :]
        side = pltpu.roll(rz[1, 1, 0:1, :], 127 - m * ni, 1)
        moved = jnp.where(
            iota((1, nk), 1) == nk - 1, jnp.concatenate([side, side], 1), pltpu.roll(row, nk - 1, 1)
        )
        for c, x in enumerate((row, moved)):
            next_row(c, m, ni, x, sharp(x))
    for q in range(nq):
        for h in range(2):
            carry = unit(ni - 1, q, h, *carry)
    c_sum, v_sum = carry
    swap(x_copies, wx.at[ni : ni + 2], wx.at[0:2], fsend.at[9], frecv.at[9], (1, 0, 0))

    def share(base, mine, value, group):
        sums[base + mine] = value
        copies = []
        for off, ids in enumerate(group):
            copy = pltpu.make_async_remote_copy(
                src_ref=sums.at[base + mine], dst_ref=sums.at[base + mine],
                send_sem=gsend.at[base + off], recv_sem=grecv.at[base + off],
                device_id=ids, device_id_type=MESH,
            )
            copy.start()
            copies.append(copy)
        return copies

    def gather(base, copies):
        for copy in copies:
            copy.wait()
        total = sums[base]
        for at in range(1, len(copies) + 1):
            total = total + sums[base + at]
        return total


    def fold(x):
        row = jnp.sum(x, axis=0, keepdims=True)
        row = row[:, :128] + row[:, 128:]
        return row + pltpu.roll(row, 64, 1)

    partial = jnp.where(iota((1, 128), 1) < 64, fold(c_sum), fold(v_sum))
    x_sums = share(0, me["gx"], partial, line)
    arrive(x_copies)

    def smooth_x(i, carry):
        lo, hi = carry
        s = 3.0 * wx[i + 2] + 2.0 * (wx[i + 1] + wx[i + 3]) + (wx[i] + wx[i + 4])
        wy[i, 8 : 8 + nj, :] = s
        for at in range(2):
            yslo[at, pl.ds(i, 1), :] = s[at : at + 1]
            yshi[at, pl.ds(i, 1), :] = s[nj - 2 + at : nj - 1 + at]
        mine = (lane >> 1) == i
        lo = jnp.where(mine, pltpu.roll(s[:, 0:128], 2 * i, 1), lo)
        hi = jnp.where(mine, pltpu.roll(s[:, nk - 128 : nk], lax.rem(2 * i + 2, 128), 1), hi)
        return lo, hi

    none = jnp.zeros((nj, 128), F32)
    lo, hi = lax.fori_loop(0, ni, smooth_x, (none, none), unroll=4)
    zslo[...] = lo
    zshi[...] = hi
    side_copies = []
    for at, (b, c) in enumerate(SIDE_STEPS):
        if c:
            rows = (slice(nj - 8, nj), slice(0, nj), slice(0, 8))[1 - b]
            to = (slice(0, 8), slice(8, 8 + nj), slice(8 + nj, 16 + nj))[1 - b]
            src = (zslo if c < 0 else zshi).at[rows]
            dst = rzz.at[1 if c < 0 else 0, to]
        else:
            src, dst = (yslo, ryhi) if b < 0 else (yshi, rylo)
        swap(side_copies, src, dst, fsend.at[at], frecv.at[at], (0, b, c))
    all_sums = share(n["gx"], me["gy"] * nz + me["gz"], gather(0, x_sums), sheet)
    arrive(side_copies)

    def smooth_rows(ref, at):
        return (
            3.0 * ref[at, 8 : 8 + nj, :]
            + 2.0 * (ref[at, 7 : 7 + nj, :] + ref[at, 9 : 9 + nj, :])
            + (ref[at, 6 : 6 + nj, :] + ref[at, 10 : 10 + nj, :])
        )

    for side in range(2):
        packs[side] = smooth_rows(rzz, side)

    def smooth_y(i, carry):
        for at in range(2):
            wy[i, 6 + at : 7 + at, :] = rylo[at, pl.ds(i, 1), :]
            wy[i, 8 + nj + at : 9 + nj + at, :] = ryhi[at, pl.ds(i, 1), :]
        out[i] = smooth_rows(wy, i)
        return carry

    lax.fori_loop(0, ni, smooth_y, 0, unroll=4)
    totals[...] = gather(n["gx"], all_sums)
    for copies in (beside, below, far, x_copies, side_copies):
        finish(copies)


def last_pass(cells, field, packs, totals, out, comp, vol):
    ni, nj, nk = field.shape
    both = totals[...]
    first = iota((1, 128), 1) < 64
    comp[0, 0] = jnp.sum(jnp.where(first, both, 0.0)) / cells
    vol[0, 0] = jnp.sum(jnp.where(first, 0.0, both)) / cells
    lanes = iota((nj, nk), 1)
    even = lax.rem(iota((nj, 128), 1), 2) == 0
    left, right = packs[0], packs[1]
    left = jnp.where(even, left + 2.0 * pltpu.roll(left, 127, 1), left)
    right = jnp.where(even, right, right + 2.0 * pltpu.roll(right, 1, 1))
    apart = jnp.abs(iota((nk, nk), 0) - iota((nk, nk), 1))
    band = jnp.maximum(3 - apart, 0).astype(F32).astype(BF16)

    def twice(x):
        return jnp.concatenate([x, x], 1)

    for i in range(ni):
        t = field[i]
        high = t.astype(BF16)
        low = (t - high.astype(F32)).astype(BF16)
        own = jnp.dot(high, band, preferred_element_type=F32) + jnp.dot(low, band, preferred_element_type=F32)
        lo = twice(pltpu.roll(left, (128 - 2 * i) % 128, 1))
        hi = twice(pltpu.roll(right, 126 - 2 * i, 1))
        out[i] = own + jnp.where(lanes < 2, lo, jnp.where(lanes >= nk - 2, hi, 0.0))


def on_device(sizes, displacement, density, stiffness):
    ni, nj, nk = density.shape
    vmem = pl.BlockSpec(memory_space=pltpu.VMEM)
    smem = pl.BlockSpec(memory_space=pltpu.SMEM)
    hbm = pl.BlockSpec(memory_space=pltpu.HBM)
    members = sizes[0] + sizes[1] * sizes[2]
    scratch = [
        displacement.shape, density.shape, stiffness.shape,
        (3, nj, nk), (3, ni, nk), (8, nk), (2, 2, nj, 128), (3, ni, nk), (8, nk), (nj, 128),
        (2, 3, ni + 1, 2, nj + 8, 128), (2, nj // 16, ni + 1, 8, nk), (6, ni, nk), (6, ni, nk), (nj, nk),
    ]
    later = [
        (ni + 4, nj, nk), (ni, nj + 16, nk),
        (2, ni, nk), (2, ni, nk), (2, ni, nk), (2, ni, nk),
        (nj, 128), (nj, 128), (2, nj + 16, 128), (members, 1, 128),
    ]
    field, packs, totals = pl.pallas_call(
        functools.partial(kernel, sizes),
        out_shape=(
            jax.ShapeDtypeStruct((ni, nj, nk), F32),
            jax.ShapeDtypeStruct((2, nj, 128), F32),
            jax.ShapeDtypeStruct((1, 128), F32),
        ),
        in_specs=[hbm] * 3,
        out_specs=(vmem, vmem, vmem),
        scratch_shapes=[pltpu.VMEM(shape, F32) for shape in scratch]
        + [pltpu.VMEM((2, nj // 16, ni + 1, 48, nk), BF16), pltpu.VMEM((192, 256), BF16)]
        + [pltpu.VMEM(shape, F32) for shape in later]
        + [pltpu.SemaphoreType.DMA((count,)) for count in (3, 7, 7, 10, 10, members, members)],
        compiler_params=pltpu.CompilerParams(
            collective_id=0, has_side_effects=True, vmem_limit_bytes=24 * 1024 * 1024
        ),
    )(*(pltpu.with_memory_space_constraint(x, pltpu.HBM) for x in (displacement, density, stiffness)))
    cells = float(ni * nj * nk * sizes[0] * sizes[1] * sizes[2])
    filtered, comp, vol = pl.pallas_call(
        functools.partial(last_pass, cells),
        out_shape=(
            jax.ShapeDtypeStruct((ni, nj, nk), F32),
            jax.ShapeDtypeStruct((1, 1), F32),
            jax.ShapeDtypeStruct((1, 1), F32),
        ),
        in_specs=[vmem] * 3,
        out_specs=(vmem, smem, smem),
        compiler_params=pltpu.CompilerParams(vmem_limit_bytes=24 * 1024 * 1024),
    )(field, packs, totals)
    return filtered, comp.reshape(()), vol.reshape(())


def solution(mesh):
    sizes = tuple(mesh.shape[axis] for axis in AXES)
    return jax.shard_map(
        functools.partial(on_device, sizes),
        mesh=mesh,
        in_specs=(P(None, "gx", "gy", "gz"), P("gx", "gy", "gz"), P()),
        out_specs=(P("gx", "gy", "gz"), P(), P()),
        check_vma=False,
    )
```

```python
import functools

import jax
import jax.numpy as jnp
from jax import lax
from jax.experimental import pallas as pl
from jax.experimental.pallas import tpu as pltpu
from jax.sharding import PartitionSpec as P

VOID = 0.001
H = (1.0, 2.0, 3.0, 2.0, 1.0)
MESH = pl.DeviceIdType.MESH
AXES = ("gx", "gy", "gz")
F32 = jnp.float32
BF16 = jnp.bfloat16
NODE_STEPS = [(a, b, c) for a in (0, 1) for b in (0, 1) for c in (0, 1) if a + b + c]
AROUND = [(a, b, c) for a in (-1, 0, 1) for b in (-1, 0, 1) for c in (-1, 0, 1) if a or b or c]


def iota(shape, dim):
    return lax.broadcasted_iota(jnp.int32, shape, dim)


def line_sum(position, extent):
    total = None
    for d in range(5):
        at = position + (d - 2)
        term = jnp.where((at >= 0) & (at < extent), H[d], 0.0).astype(F32)
        total = term if total is None else total + term
    return total


def band_weights(stiff):
    rows, cols = 192, 128
    pick = jnp.where((iota((rows, 24), 0) >> 3) == iota((rows, 24), 1), 1.0, 0.0).astype(F32)

    def column(shape):
        col = iota(shape, 1)
        a, m, s = col >> 6, (col >> 4) & 3, col & 15
        edge = m == 3
        c = jnp.where(edge, jnp.where(s >= 3, 1, 0), s >> 3)
        m = jnp.where(edge, s - 3 * c, m)
        valid = jnp.logical_not(edge) | (s < 6)
        return 8 * m + 4 * a + c, valid, jnp.where(edge, 8, s & 7)

    total = None
    for b in (0, 1):
        q, valid, _ = column((24, cols))
        place = jnp.where((iota((24, cols), 0) == q + 2 * b) & valid, 1.0, 0.0).astype(F32)
        wide = jnp.dot(stiff, place, precision=lax.Precision.HIGHEST, preferred_element_type=F32)
        tall = jnp.dot(pick, wide, precision=lax.Precision.HIGHEST, preferred_element_type=F32)
        _, _, jj = column((rows, cols))
        term = jnp.where(jj - (iota((rows, cols), 0) & 7) == b, tall, 0.0)
        total = term if total is None else total + term
    high = total.astype(BF16)
    return jnp.concatenate([high, (total - high.astype(F32)).astype(BF16)], 1)


def kernel(
    sizes, u_hbm, rho_hbm, stiff_hbm, out, totals,
    u, rho, stiff, rx, ry, rxy, rz, ys, yd, zs,
    field, edge, line_f, line_u, inv, parts, weights, band, wx, wy,
    ysend, corner_send, zsend, rows_in, corner_in, rzz, rzs, yrow,
    sums, insem, nsend, nrecv, fsend, frecv, gsend, grecv,
):
    ni, nj, nk = rho.shape
    n = dict(zip(AXES, sizes))
    me = {axis: lax.axis_index(axis) for axis in AXES}
    ny, nz = n["gy"], n["gz"]
    down = {axis: me[axis] > 0 for axis in AXES}
    up = {axis: me[axis] < n[axis] - 1 for axis in AXES}

    loads = []
    for at, (src, dst) in enumerate(((stiff_hbm, stiff), (u_hbm, u), (rho_hbm, rho))):
        copy = pltpu.make_async_copy(src, dst, insem.at[at])
        copy.start()
        loads.append(copy)

    def hop(step):
        ids, ok = {}, None
        for axis, s in zip(AXES, step):
            if s:
                ids[axis] = me[axis] + s
                flag = up[axis] if s > 0 else down[axis]
                ok = flag if ok is None else jnp.logical_and(ok, flag)
        return ids, ok

    def minus(step):
        return tuple(-s for s in step)

    line = [{"gx": lax.rem(me["gx"] + off, n["gx"])} for off in range(1, n["gx"])]
    sheet = [
        {"gy": lax.rem(me["gy"] + off // nz, ny), "gz": lax.rem(me["gz"] + off % nz, nz)}
        for off in range(1, ny * nz)
    ]
    barrier = pltpu.get_barrier_semaphore()
    for ids in line + sheet:
        pl.semaphore_signal(barrier, inc=1, device_id=ids, device_id_type=MESH)
    peers = len(line) + len(sheet)
    for step in AROUND:
        if step[0] and (step[1] or step[2]):
            ids, ok = hop(step)
            peers = peers + jnp.where(ok, 1, 0)

            @pl.when(ok)
            def _():
                pl.semaphore_signal(barrier, inc=1, device_id=ids, device_id_type=MESH)

    def node_route(step):
        a, b, c = step
        if c:
            return (zs.at[0:8], rz.at[a, b, 0:8]) if b else (zs, rz.at[a, b])
        if b:
            return (yd, rxy) if a else (ys, ry)
        return u_hbm.at[:, 0], rx

    def face_route(step):
        a, b, c = step
        hi_a, hi_b, hi_c = a > 0, b > 0, c > 0
        if c:
            rows = (slice(nj - 8, nj), slice(0, nj), slice(0, 8))[1 - b]
            to = (slice(0, 8), slice(8, 8 + nj), slice(8 + nj, 16 + nj))[1 - b]
            return zsend.at[int(hi_c), rows], rzz.at[1 - hi_c, 1 - a, to]
        if a and b:
            return corner_send.at[int(hi_a), int(hi_b)], corner_in.at[1 - hi_a, 1 - hi_b]
        if b:
            at = 2 * (1 - hi_b)
            return ysend.at[int(hi_b)], rows_in.at[at : at + 2, 8 : 8 + ni]
        return (wx.at[ni : ni + 2], wx.at[0:2]) if hi_a else (wx.at[2:4], wx.at[ni + 2 : ni + 4])

    def clear(dst, step):
        @pl.when(jnp.logical_not(hop(step)[1]))
        def _():
            dst[...] = jnp.zeros(dst.shape, F32)

    for step in NODE_STEPS:
        clear(node_route(step)[1], step)
    for step in AROUND:
        clear(face_route(step)[1], minus(step))
    apart = jnp.abs(iota((nk, nk), 0) - iota((nk, nk), 1))
    band[...] = jnp.maximum(3 - apart, 0).astype(F32).astype(BF16)
    edge[...] = jnp.zeros(edge.shape, F32)

    pl.semaphore_wait(barrier, peers)

    def swap(copies, src, dst, send_sem, recv_sem, step):
        ids, sends = hop(step)
        copy = pltpu.make_async_remote_copy(
            src_ref=src, dst_ref=dst, send_sem=send_sem, recv_sem=recv_sem,
            device_id=ids, device_id_type=MESH,
        )
        copies.append((copy, sends, hop(minus(step))[1]))

        @pl.when(sends)
        def _():
            copy.start()

    def arrive(copies):
        for copy, _, takes in copies:

            @pl.when(takes)
            def _():
                copy.wait_recv()

    def finish(copies):
        for copy, sends, _ in copies:

            @pl.when(sends)
            def _():
                copy.wait_send()

    beside, below, far = [], [], []

    def node_swap(step):
        a, b, c = step
        at = NODE_STEPS.index(step)
        src, dst = node_route(step)
        copies = far if a else (below if b else beside)
        swap(copies, src, dst, nsend.at[at], nrecv.at[at], minus(step))

    def face_swap(copies, step):
        at = AROUND.index(step)
        src, dst = face_route(step)
        swap(copies, src, dst, fsend.at[at], frecv.at[at], step)

    node_swap((1, 0, 0))
    loads[0].wait()
    weights[...] = band_weights(stiff[...])
    loads[1].wait()
    lane = iota((nj, 128), 1)
    packed = jnp.zeros((nj, 128), F32)
    for at in range(3 * ni):
        column = u[at // ni, at % ni, :, 0:128]
        packed = jnp.where(lane == at, pltpu.roll(column, at, 1) if at else column, packed)
    zs[...] = packed
    for step in NODE_STEPS:
        if step[2]:
            node_swap(step)
    yd[...] = jnp.zeros(yd.shape, F32)
    for m in range(3):
        for i in range(ni):
            ys[m, i : i + 1, :] = u[m, i, 0:1, :]
        yd[m : m + 1, :] = u[m, 0, 0:1, :]
    node_swap((0, 1, 0))
    node_swap((1, 1, 0))

    last = iota((nj, 128), 1) == 127
    nq = nj // 16

    def sharp(x):
        return x + (x - x.astype(BF16).astype(F32))

    def pair(x, q):
        return jnp.concatenate([x[16 * q : 16 * q + 8], x[16 * q + 8 : 16 * q + 16]], 1)

    def layer(h, to, at, source, col):
        for m in range(3):
            x = source(m, h)
            side = source(m, 1) if h == 0 else col
            turn = 127 if h == 0 else 127 - (m * ni + at)
            moved = jnp.where(last, pltpu.roll(side, turn, 1), pltpu.roll(x, 127, 1))
            for c, y in enumerate((x, moved)):
                field[c, m, to, h, 0:nj, :] = sharp(y)
                for jt in range(nj // 8 - 1):
                    edge[h, jt // 2, to, 3 * c + m : 3 * c + m + 1, 128 * (jt % 2) : 128 * (jt % 2) + 128] = (
                        y[8 * jt + 8 : 8 * jt + 9, :]
                    )
            for q in range(nq):
                parts[h, q, to, 16 * m : 16 * m + 16, :] = jnp.concatenate([pair(x, q), pair(moved, q)], 0).astype(BF16)

    def own(i):
        return lambda m, h: u[m, i, :, 128 * h : 128 * h + 128]

    def next_row(c, m, to, x, f):
        for h in range(2):
            half = slice(128 * h, 128 * h + 128)
            field[c, m, to, h, nj : nj + 1, :] = f[:, half]
            edge[h, nq - 1, to, 3 * c + m : 3 * c + m + 1, 128:256] = x[:, half]

    def own_row(i, carry):
        for c in range(2):
            for m in range(3):
                at = pl.ds(i, 1)
                next_row(c, m, i, line_u[3 * c + m, at, :], line_f[3 * c + m, at, :])
        return carry

    none8 = jnp.zeros((8, nk), F32)

    def tile(h, q, p):
        return [parts[h, q, p], jnp.concatenate([edge[h, q, p], none8], 0).astype(BF16)]

    def unit(i, q, h, c_sum, v_sum):
        half = slice(128 * h, 128 * h + 128)
        rows = [slice(16 * q + 8 * t, 16 * q + 8 * t + 8) for t in range(2)]
        data = tile(h, q, i) + tile(h, q, i + 1)
        product = jnp.dot(weights[...], jnp.concatenate(data + data, 0), preferred_element_type=F32)
        energy = None
        for r in range(24):
            m, a, b, c = r >> 3, (r >> 2) & 1, (r >> 1) & 1, r & 1
            f = [field[c, m, i + a, h, 16 * q + 8 * t + b : 16 * q + 8 * t + b + 8, :] for t in range(2)]
            term = product[8 * r : 8 * r + 8] * jnp.concatenate(f, 1)
            energy = term if energy is None else energy + term
        d = jnp.concatenate([rho[i, rows[t], half] for t in range(2)], 1)
        scale = jnp.concatenate([inv[rows[t], half] for t in range(2)], 1)
        inv_x = 1.0 / line_sum(jnp.full((8, nk), me["gx"] * ni + i, jnp.int32), n["gx"] * ni)
        w = (-3.0 * (1.0 - VOID)) * d * d * energy * (inv_x * scale)
        for t in range(2):
            wx[i + 2, rows[t], half] = w[:, 128 * t : 128 * t + 128]
        return c_sum + (VOID + d * d * d * (1.0 - VOID)) * energy, v_sum + d

    def sweep(h):
        def body(i, carry):
            layer(h, i + 1, i + 1, own(i + 1), rz[0, 0])
            return unit(i, 0, h, *carry)

        return body

    loads[2].wait()
    inv[...] = 1.0 / (
        line_sum(me["gy"] * nj + iota((nj, nk), 0), ny * nj)
        * line_sum(me["gz"] * nk + iota((nj, nk), 1), nz * nk)
    )
    carry = (none8, none8)
    layer(0, 0, 0, own(0), None)
    carry = lax.fori_loop(0, ni - 1, sweep(0), carry, unroll=5)
    arrive(beside)
    layer(1, 0, 0, own(0), rz[0, 0])
    carry = lax.fori_loop(0, ni - 1, sweep(1), carry, unroll=5)
    arrive(below)
    for m in range(3):
        base = ry[m]
        mine = iota((ni, 128), 1) == iota((ni, 128), 0) + m * ni
        corner = jnp.sum(jnp.where(mine, rz[0, 1, 0:1, :], 0.0), axis=1, keepdims=True)
        moved = jnp.where(iota((ni, nk), 1) == nk - 1, corner, pltpu.roll(base, nk - 1, 1))
        for c, x in enumerate((base, moved)):
            line_u[3 * c + m] = x
            line_f[3 * c + m] = sharp(x)
    lax.fori_loop(0, ni, own_row, 0, unroll=4)

    def upper(i, carry):
        for q in range(1, nq):
            for h in range(2):
                carry = unit(i, q, h, *carry)
        return carry

    carry = lax.fori_loop(0, ni - 1, upper, carry, unroll=5)
    around = []
    face_swap(around, (-1, 0, 0))
    arrive(far)
    for h in range(2):
        layer(h, ni, 0, lambda m, h: rx[m, :, 128 * h : 128 * h + 128], rz[1, 0])
    for m in range(3):
        row = rxy[m : m + 1, :]
        side = pltpu.roll(rz[1, 1, 0:1, :], 127 - m * ni, 1)
        moved = jnp.where(
            iota((1, nk), 1) == nk - 1, jnp.concatenate([side, side], 1), pltpu.roll(row, nk - 1, 1)
        )
        for c, x in enumerate((row, moved)):
            next_row(c, m, ni, x, sharp(x))
    for q in range(nq):
        for h in range(2):
            carry = unit(ni - 1, q, h, *carry)
    c_sum, v_sum = carry
    face_swap(around, (1, 0, 0))

    def share(base, mine, value, group):
        sums[base + mine] = value
        copies = []
        for off, ids in enumerate(group):
            copy = pltpu.make_async_remote_copy(
                src_ref=sums.at[base + mine], dst_ref=sums.at[base + mine],
                send_sem=gsend.at[base + off], recv_sem=grecv.at[base + off],
                device_id=ids, device_id_type=MESH,
            )
            copy.start()
            copies.append(copy)
        return copies

    def gather(base, copies):
        for copy in copies:
            copy.wait()
        total = sums[base]
        for at in range(1, len(copies) + 1):
            total = total + sums[base + at]
        return total


    def fold(x):
        row = jnp.sum(x, axis=0, keepdims=True)
        row = row[:, :128] + row[:, 128:]
        return row + pltpu.roll(row, 64, 1)

    partial = jnp.where(iota((1, 128), 1) < 64, fold(c_sum), fold(v_sum))
    x_sums = share(0, me["gx"], partial, line)

    zlo = zhi = jnp.zeros((nj, 128), F32)
    for i in range(ni):
        mine = (lane >> 1) == i + 2
        plane = wx[i + 2]
        zlo = jnp.where(mine, pltpu.roll(plane[:, 0:128], 2 * i + 4, 1), zlo)
        zhi = jnp.where(mine, pltpu.roll(plane[:, nk - 128 : nk], (2 * i + 6) % 128, 1), zhi)
        for t in range(2):
            for top, row in enumerate((t, nj - 2 + t)):
                line_at = wx[i + 2, row : row + 1, :]
                ysend[top, t, i : i + 1, :] = line_at
                if i < 2 or i >= ni - 2:
                    p = i if i < 2 else i - ni + 2
                    corner_send[int(i >= 2), top, 2 * p + t : 2 * p + t + 1, :] = line_at
    zsend[0] = zlo
    zsend[1] = zhi
    for step in AROUND:
        if step[1] or step[2]:
            face_swap(around, step)

    def spread_x(i):
        return 3.0 * wx[i + 2] + 2.0 * (wx[i + 1] + wx[i + 3]) + (wx[i] + wx[i + 4])

    def spread_z(xs):
        x = jnp.concatenate(xs, 0)
        high = x.astype(BF16)
        low = (x - high.astype(F32)).astype(BF16)
        both = jnp.dot(jnp.concatenate([high, low], 0), band[...], preferred_element_type=F32)
        return both[: x.shape[0]] + both[x.shape[0] :]

    def planes_xz(group):
        done = spread_z([spread_x(i) for i in group])
        for at, i in enumerate(group):
            for h in range(2):
                wy[i, h, 8 : 8 + nj, :] = done[nj * at : nj * at + nj, 128 * h : 128 * h + 128]

    for first in range(2, ni - 2, 4):
        planes_xz(range(first, min(first + 4, ni - 2)))
    all_sums = share(n["gx"], me["gy"] * nz + me["gz"], gather(0, x_sums), sheet)
    arrive(around)

    planes_xz((0, 1, ni - 2, ni - 1))
    lines = []
    for at in range(4):
        side, t = at >> 1, at & 1
        for p in range(2):
            rows_in[at, 6 + p : 7 + p, :] = corner_in[0, side, 2 * p + t : 2 * p + t + 1, :]
            rows_in[at, 8 + ni + p : 9 + ni + p, :] = corner_in[1, side, 2 * p + t : 2 * p + t + 1, :]
        x = [rows_in[at, 6 + d : 6 + d + ni, :] for d in range(5)]
        lines.append(3.0 * x[2] + 2.0 * (x[1] + x[3]) + (x[0] + x[4]))
    done = spread_z(lines)
    for at in range(4):
        yrow[at] = done[ni * at : ni * at + ni]

    wide = iota((nj + 16, 128), 1)
    even = lax.rem(lane, 2) == 0
    rims = []
    for side in range(2):
        x = jnp.where(
            wide < 4,
            pltpu.roll(rzz[side, 0], 128 - 2 * ni, 1),
            jnp.where(wide < 2 * ni + 4, rzz[side, 1], pltpu.roll(rzz[side, 2], 2 * ni, 1)),
        )
        x = (
            3.0 * x
            + 2.0 * (pltpu.roll(x, 2, 1) + pltpu.roll(x, 126, 1))
            + (pltpu.roll(x, 4, 1) + pltpu.roll(x, 124, 1))
        )
        rzs[side] = x
        y = [rzs[side, 6 + d : 6 + d + nj, :] for d in range(5)]
        y = 3.0 * y[2] + 2.0 * (y[1] + y[3]) + (y[0] + y[4])
        y = y + jnp.where(even, 0.0, 2.0 * pltpu.roll(y, 1, 1)) if side else (
            y + jnp.where(even, 2.0 * pltpu.roll(y, 127, 1), 0.0)
        )
        rims.append(y)

    for i in range(ni):
        for h in range(2):
            half = slice(128 * h, 128 * h + 128)
            for t in range(2):
                wy[i, h, 6 + t : 7 + t, :] = yrow[t, i : i + 1, half]
                wy[i, h, 8 + nj + t : 9 + nj + t, :] = yrow[2 + t, i : i + 1, half]
            y = [wy[i, h, 6 + d : 6 + d + nj, :] for d in range(5)]
            y = 3.0 * y[2] + 2.0 * (y[1] + y[3]) + (y[0] + y[4])
            if h:
                rim = jnp.where(lane >= 126, pltpu.roll(rims[1], 122 - 2 * i, 1), 0.0)
            else:
                rim = jnp.where(lane < 2, pltpu.roll(rims[0], 124 - 2 * i, 1), 0.0)
            out[i, :, half] = y + rim
    totals[...] = gather(n["gx"], all_sums)
    for copies in (beside, below, far, around):
        finish(copies)


def last_pass(cells, field, totals, out, comp, vol, sem):
    copy = pltpu.make_async_copy(field, out, sem.at[0])
    copy.start()
    both = totals[...]
    first = iota((1, 128), 1) < 64
    comp[0, 0] = jnp.sum(jnp.where(first, both, 0.0)) / cells
    vol[0, 0] = jnp.sum(jnp.where(first, 0.0, both)) / cells
    copy.wait()


def on_device(sizes, displacement, density, stiffness):
    ni, nj, nk = density.shape
    vmem = pl.BlockSpec(memory_space=pltpu.VMEM)
    smem = pl.BlockSpec(memory_space=pltpu.SMEM)
    hbm = pl.BlockSpec(memory_space=pltpu.HBM)
    members = sizes[0] + sizes[1] * sizes[2]
    scratch = [
        displacement.shape, density.shape, stiffness.shape,
        (3, nj, nk), (3, ni, nk), (8, nk), (2, 2, nj, 128), (3, ni, nk), (8, nk), (nj, 128),
        (2, 3, ni + 1, 2, nj + 8, 128), (2, nj // 16, ni + 1, 8, nk), (6, ni, nk), (6, ni, nk), (nj, nk),
    ]
    later = [
        (ni + 4, nj, nk), (ni, 2, nj + 16, 128),
        (2, 2, ni, nk), (2, 2, 8, nk), (2, nj, 128), (4, ni + 16, nk), (2, 2, 8, nk),
        (2, 3, nj + 16, 128), (2, nj + 16, 128), (4, ni, nk), (members, 1, 128),
    ]
    field, totals = pl.pallas_call(
        functools.partial(kernel, sizes),
        out_shape=(
            jax.ShapeDtypeStruct((ni, nj, nk), F32),
            jax.ShapeDtypeStruct((1, 128), F32),
        ),
        in_specs=[hbm] * 3,
        out_specs=(vmem, vmem),
        scratch_shapes=[pltpu.VMEM(shape, F32) for shape in scratch]
        + [pltpu.VMEM((2, nj // 16, ni + 1, 48, nk), BF16), pltpu.VMEM((192, 256), BF16), pltpu.VMEM((nk, nk), BF16)]
        + [pltpu.VMEM(shape, F32) for shape in later]
        + [pltpu.SemaphoreType.DMA((count,)) for count in (3, 7, 7, 26, 26, members, members)],
        compiler_params=pltpu.CompilerParams(
            collective_id=0, has_side_effects=True, vmem_limit_bytes=24 * 1024 * 1024
        ),
    )(*(pltpu.with_memory_space_constraint(x, pltpu.HBM) for x in (displacement, density, stiffness)))
    cells = float(ni * nj * nk * sizes[0] * sizes[1] * sizes[2])
    filtered, comp, vol = pl.pallas_call(
        functools.partial(last_pass, cells),
        out_shape=(
            jax.ShapeDtypeStruct((ni, nj, nk), F32),
            jax.ShapeDtypeStruct((1, 1), F32),
            jax.ShapeDtypeStruct((1, 1), F32),
        ),
        in_specs=[vmem] * 2,
        out_specs=(hbm, smem, smem),
        scratch_shapes=[pltpu.SemaphoreType.DMA((1,))],
        compiler_params=pltpu.CompilerParams(vmem_limit_bytes=24 * 1024 * 1024),
    )(field, totals)
    return filtered, comp.reshape(()), vol.reshape(())


def solution(mesh):
    sizes = tuple(mesh.shape[axis] for axis in AXES)
    return jax.shard_map(
        functools.partial(on_device, sizes),
        mesh=mesh,
        in_specs=(P(None, "gx", "gy", "gz"), P("gx", "gy", "gz"), P()),
        out_specs=(P("gx", "gy", "gz"), P(), P()),
        check_vma=False,
    )
```

```python
import functools

import jax
import jax.numpy as jnp
from jax import lax
from jax.experimental import pallas as pl
from jax.experimental.pallas import tpu as pltpu
from jax.sharding import PartitionSpec as P

VOID = 0.001
H = (1.0, 2.0, 3.0, 2.0, 1.0)
MESH = pl.DeviceIdType.MESH
AXES = ("gx", "gy", "gz")
F32 = jnp.float32
BF16 = jnp.bfloat16
NODE_STEPS = [(a, b, c) for a in (0, 1) for b in (0, 1) for c in (0, 1) if a + b + c]
FEW = 64
AROUND = [(a, b, c) for a in (-1, 0, 1) for b in (-1, 0, 1) for c in (-1, 0, 1) if a or b or c]


def iota(shape, dim):
    return lax.broadcasted_iota(jnp.int32, shape, dim)


def line_sum(position, extent):
    total = None
    for d in range(5):
        at = position + (d - 2)
        term = jnp.where((at >= 0) & (at < extent), H[d], 0.0).astype(F32)
        total = term if total is None else total + term
    return total


def band_weights(stiff):
    rows, cols = 192, 128
    pick = jnp.where((iota((rows, 24), 0) >> 3) == iota((rows, 24), 1), 1.0, 0.0).astype(F32)

    def column(shape):
        col = iota(shape, 1)
        a, m, s = col >> 6, (col >> 4) & 3, col & 15
        edge = m == 3
        c = jnp.where(edge, jnp.where(s >= 3, 1, 0), s >> 3)
        m = jnp.where(edge, s - 3 * c, m)
        valid = jnp.logical_not(edge) | (s < 6)
        return 8 * m + 4 * a + c, valid, jnp.where(edge, 8, s & 7)

    total = None
    for b in (0, 1):
        q, valid, _ = column((24, cols))
        place = jnp.where((iota((24, cols), 0) == q + 2 * b) & valid, 1.0, 0.0).astype(F32)
        wide = jnp.dot(stiff, place, precision=lax.Precision.HIGHEST, preferred_element_type=F32)
        tall = jnp.dot(pick, wide, precision=lax.Precision.HIGHEST, preferred_element_type=F32)
        _, _, jj = column((rows, cols))
        term = jnp.where(jj - (iota((rows, cols), 0) & 7) == b, tall, 0.0)
        total = term if total is None else total + term
    high = total.astype(BF16)
    return jnp.concatenate([high, (total - high.astype(F32)).astype(BF16)], 1)


def kernel(
    sizes, u_hbm, rho_hbm, stiff_hbm, out, totals,
    u, rho, stiff, rx, ry, rxy, rz, ys, yd, zs,
    field, edge, line_f, line_u, inv, parts, weights, band, wx, wy,
    ysend, corner_send, zsend, rows_in, corner_in, rzz, rzs, yrow,
    sums, insem, nsend, nrecv, fsend, frecv, gsend, grecv, known,
):
    ni, nj, nk = rho.shape
    n = dict(zip(AXES, sizes))
    me = {axis: lax.axis_index(axis) for axis in AXES}
    ny, nz = n["gy"], n["gz"]
    down = {axis: me[axis] > 0 for axis in AXES}
    up = {axis: me[axis] < n[axis] - 1 for axis in AXES}

    loads = []
    halves = [(u_hbm.at[:, :, :, at : at + 128], u.at[:, :, :, at : at + 128]) for at in (0, 128)]
    for at, (src, dst) in enumerate([(stiff_hbm, stiff)] + halves + [(rho_hbm, rho)]):
        copy = pltpu.make_async_copy(src, dst, insem.at[at])
        copy.start()
        loads.append(copy)

    def hop(step):
        ids, ok = {}, None
        for axis, s in zip(AXES, step):
            if s:
                ids[axis] = me[axis] + s
                flag = up[axis] if s > 0 else down[axis]
                ok = flag if ok is None else jnp.logical_and(ok, flag)
        return ids, ok

    def minus(step):
        return tuple(-s for s in step)

    everyone = n["gx"] * ny * nz
    mine = (me["gx"] * ny + me["gy"]) * nz + me["gz"]

    def place(at):
        return {"gx": at // (ny * nz), "gy": lax.rem(at // nz, ny), "gz": lax.rem(at, nz)}

    line = [{"gx": lax.rem(me["gx"] + off, n["gx"])} for off in range(1, n["gx"])]
    sheet = [
        {"gy": lax.rem(me["gy"] + off // nz, ny), "gz": lax.rem(me["gz"] + off % nz, nz)}
        for off in range(1, ny * nz)
    ]
    if everyone <= FEW:
        group = [place(lax.rem(mine + off, everyone)) for off in range(1, everyone)]
        stages = [(mine, group)]
        met = [(ids, True, mine + off < everyone) for off, ids in enumerate(group, 1)]
    else:
        stages = [(me["gx"], line), (me["gy"] * nz + me["gz"], sheet)]
        met = [(ids, True, me["gx"] + off < n["gx"]) for off, ids in enumerate(line, 1)]
        met += [(ids, True, me["gy"] * nz + me["gz"] + off < ny * nz) for off, ids in enumerate(sheet, 1)]
        met += [hop(step) + (step[0] > 0,) for step in AROUND if step[0] and (step[1] or step[2])]

    def greet(semaphore, upward):
        for ids, ok, later in met:
            flag = later if upward else jnp.logical_not(later)

            @pl.when(jnp.logical_and(ok, flag))
            def _():
                pl.semaphore_signal(semaphore, inc=1, device_id=ids, device_id_type=MESH)

    def count(upward):
        total = 0
        for _, ok, later in met:
            flag = later if upward else jnp.logical_not(later)
            total = total + jnp.where(jnp.logical_and(ok, flag), 1, 0)
        return total

    def hear(semaphore, amount):
        @pl.when(amount > 0)
        def _():
            pl.semaphore_wait(semaphore, amount)

    barrier = pltpu.get_barrier_semaphore()
    greet(barrier, True)

    def node_route(step):
        a, b, c = step
        if c:
            return (zs.at[0:8], rz.at[a, b, 0:8]) if b else (zs, rz.at[a, b])
        if b:
            return (yd, rxy) if a else (ys, ry)
        return u.at[:, 0], rx

    def face_route(step):
        a, b, c = step
        hi_a, hi_b, hi_c = a > 0, b > 0, c > 0
        if c:
            rows = (slice(nj - 8, nj), slice(0, nj), slice(0, 8))[1 - b]
            to = (slice(0, 8), slice(8, 8 + nj), slice(8 + nj, 16 + nj))[1 - b]
            return zsend.at[int(hi_c), rows], rzz.at[1 - hi_c, 1 - a, to]
        if a and b:
            return corner_send.at[int(hi_a), int(hi_b)], corner_in.at[1 - hi_a, 1 - hi_b]
        if b:
            at = 2 * (1 - hi_b)
            return ysend.at[int(hi_b)], rows_in.at[at : at + 2, 8 : 8 + ni]
        return (wx.at[ni : ni + 2], wx.at[0:2]) if hi_a else (wx.at[2:4], wx.at[ni + 2 : ni + 4])

    def clear(dst, step):
        @pl.when(jnp.logical_not(hop(step)[1]))
        def _():
            dst[...] = jnp.zeros(dst.shape, F32)

    for step in NODE_STEPS:
        clear(node_route(step)[1], step)
    for step in AROUND:
        clear(face_route(step)[1], minus(step))
    apart = jnp.abs(iota((nk, nk), 0) - iota((nk, nk), 1))
    band[...] = jnp.maximum(3 - apart, 0).astype(F32).astype(BF16)
    edge[...] = jnp.zeros(edge.shape, F32)

    def swap(copies, src, dst, send_sem, recv_sem, step):
        ids, sends = hop(step)
        copy = pltpu.make_async_remote_copy(
            src_ref=src, dst_ref=dst, send_sem=send_sem, recv_sem=recv_sem,
            device_id=ids, device_id_type=MESH,
        )
        copies.append((copy, sends, hop(minus(step))[1]))

        @pl.when(sends)
        def _():
            copy.start()

    def arrive(copies):
        for copy, _, takes in copies:

            @pl.when(takes)
            def _():
                copy.wait_recv()

    def finish(copies):
        for copy, sends, _ in copies:

            @pl.when(sends)
            def _():
                copy.wait_send()

    beside, below, far = [], [], []

    def node_swap(step):
        a, b, c = step
        at = NODE_STEPS.index(step)
        src, dst = node_route(step)
        copies = far if a else (below if b else beside)
        swap(copies, src, dst, nsend.at[at], nrecv.at[at], minus(step))

    def face_swap(copies, step):
        at = AROUND.index(step)
        src, dst = face_route(step)
        swap(copies, src, dst, fsend.at[at], frecv.at[at], step)

    loads[0].wait()
    weights[...] = band_weights(stiff[...])
    loads[1].wait()
    lane = iota((nj, 128), 1)
    packed = jnp.zeros((nj, 128), F32)
    for at in range(3 * ni):
        column = u[at // ni, at % ni, :, 0:128]
        packed = jnp.where(lane == at, pltpu.roll(column, at, 1) if at else column, packed)
    zs[...] = packed
    loads[2].wait()
    yd[...] = jnp.zeros(yd.shape, F32)
    for m in range(3):
        for i in range(ni):
            ys[m, i : i + 1, :] = u[m, i, 0:1, :]
        yd[m : m + 1, :] = u[m, 0, 0:1, :]
    hear(barrier, mine if everyone <= FEW else count(False))
    for step in sorted(NODE_STEPS, key=lambda step: (sum(step), step)):
        node_swap(step)
    greet(known.at[0], False)

    last = iota((nj, 128), 1) == 127
    nq = nj // 16

    def sharp(x):
        return x + (x - x.astype(BF16).astype(F32))

    def pair(x, q):
        return jnp.concatenate([x[16 * q : 16 * q + 8], x[16 * q + 8 : 16 * q + 16]], 1)

    def layer(h, to, at, source, col):
        for m in range(3):
            x = source(m, h)
            side = source(m, 1) if h == 0 else col
            turn = 127 if h == 0 else 127 - (m * ni + at)
            moved = jnp.where(last, pltpu.roll(side, turn, 1), pltpu.roll(x, 127, 1))
            for c, y in enumerate((x, moved)):
                field[c, m, to, h, 0:nj, :] = sharp(y)
                for jt in range(nj // 8 - 1):
                    edge[h, jt // 2, to, 3 * c + m : 3 * c + m + 1, 128 * (jt % 2) : 128 * (jt % 2) + 128] = (
                        y[8 * jt + 8 : 8 * jt + 9, :]
                    )
            for q in range(nq):
                parts[h, q, to, 16 * m : 16 * m + 16, :] = jnp.concatenate([pair(x, q), pair(moved, q)], 0).astype(BF16)

    def own(i):
        return lambda m, h: u[m, i, :, 128 * h : 128 * h + 128]

    def next_row(c, m, to, h, x):
        field[c, m, to, h, nj : nj + 1, :] = sharp(x)
        edge[h, nq - 1, to, 3 * c + m : 3 * c + m + 1, 128:256] = x

    def own_row(i, carry):
        at = pl.ds(i, 1)
        for h in range(2):
            for cm in range(6):
                field[cm // 3, cm % 3, i, h, nj : nj + 1, :] = line_f[h, cm, at, :]
                edge[h, nq - 1, i, cm : cm + 1, 128:256] = line_u[h, cm, at, :]
        return carry

    none8 = jnp.zeros((8, nk), F32)

    def tile(h, q, p):
        return [parts[h, q, p], jnp.concatenate([edge[h, q, p], none8], 0).astype(BF16)]

    def unit(i, q, h, c_sum, v_sum):
        half = slice(128 * h, 128 * h + 128)
        rows = [slice(16 * q + 8 * t, 16 * q + 8 * t + 8) for t in range(2)]
        data = tile(h, q, i) + tile(h, q, i + 1)
        product = jnp.dot(weights[...], jnp.concatenate(data + data, 0), preferred_element_type=F32)
        energy = None
        for r in range(24):
            m, a, b, c = r >> 3, (r >> 2) & 1, (r >> 1) & 1, r & 1
            f = [field[c, m, i + a, h, 16 * q + 8 * t + b : 16 * q + 8 * t + b + 8, :] for t in range(2)]
            term = product[8 * r : 8 * r + 8] * jnp.concatenate(f, 1)
            energy = term if energy is None else energy + term
        d = jnp.concatenate([rho[i, rows[t], half] for t in range(2)], 1)
        scale = jnp.concatenate([inv[rows[t], half] for t in range(2)], 1)
        inv_x = 1.0 / line_sum(jnp.full((8, nk), me["gx"] * ni + i, jnp.int32), n["gx"] * ni)
        w = (-3.0 * (1.0 - VOID)) * d * d * energy * (inv_x * scale)
        for t in range(2):
            wx[i + 2, rows[t], half] = w[:, 128 * t : 128 * t + 128]
        return c_sum + (VOID + d * d * d * (1.0 - VOID)) * energy, v_sum + d

    def sweep(h):
        def body(i, carry):
            layer(h, i + 1, i + 1, own(i + 1), rz[0, 0])
            return unit(i, 0, h, *carry)

        return body

    loads[3].wait()
    inv[...] = 1.0 / (
        line_sum(me["gy"] * nj + iota((nj, nk), 0), ny * nj)
        * line_sum(me["gz"] * nk + iota((nj, nk), 1), nz * nk)
    )
    carry = (none8, none8)
    layer(0, 0, 0, own(0), None)
    carry = lax.fori_loop(0, ni - 1, sweep(0), carry, unroll=5)
    arrive(beside)
    layer(1, 0, 0, own(0), rz[0, 0])
    carry = lax.fori_loop(0, ni - 1, sweep(1), carry, unroll=5)
    arrive(below)

    def row_pair(h):
        for m in range(3):
            base = ry[m]
            if h:
                mine = iota((ni, 128), 1) == iota((ni, 128), 0) + m * ni
                side = jnp.sum(jnp.where(mine, rz[0, 1, 0:1, :], 0.0), axis=1, keepdims=True)
            else:
                side = pltpu.roll(base[:, 128:256], 127, 1)
            x = base[:, 128 * h : 128 * h + 128]
            moved = jnp.where(iota((ni, 128), 1) == 127, side, pltpu.roll(x, 127, 1))
            for c, y in enumerate((x, moved)):
                line_u[h, 3 * c + m] = y
                line_f[h, 3 * c + m] = sharp(y)

    def upper(i, carry):
        for q in range(1, nq):
            for h in range(2):
                carry = unit(i, q, h, *carry)
        return carry

    for h in range(2):
        row_pair(h)
    lax.fori_loop(0, ni, own_row, 0, unroll=4)
    carry = lax.fori_loop(0, ni - 1, upper, carry, unroll=5)
    zlo = zhi = jnp.zeros((nj, 128), F32)

    def pack(i, zlo, zhi):
        slot = (lane >> 1) == i + 2
        plane = wx[i + 2]
        zlo = jnp.where(slot, pltpu.roll(plane[:, 0:128], 2 * i + 4, 1), zlo)
        zhi = jnp.where(slot, pltpu.roll(plane[:, nk - 128 : nk], (2 * i + 6) % 128, 1), zhi)
        for t in range(2):
            for top, row in enumerate((t, nj - 2 + t)):
                line_at = wx[i + 2, row : row + 1, :]
                ysend[top, t, i : i + 1, :] = line_at
                if i < 2 or i >= ni - 2:
                    p = i if i < 2 else i - ni + 2
                    corner_send[int(i >= 2), top, 2 * p + t : 2 * p + t + 1, :] = line_at
        return zlo, zhi

    for i in range(ni - 1):
        zlo, zhi = pack(i, zlo, zhi)
    zsend[0] = zlo
    zsend[1] = zhi
    hear(known.at[0], everyone - 1 - mine if everyone <= FEW else count(True))
    around = []
    face_swap(around, (-1, 0, 0))
    arrive(far)
    for h in range(2):
        layer(h, ni, 0, lambda m, h: rx[m, :, 128 * h : 128 * h + 128], rz[1, 0])
    for m in range(3):
        row = rxy[m : m + 1, :]
        side = pltpu.roll(rz[1, 1, 0:1, :], 127 - m * ni, 1)
        moved = jnp.where(
            iota((1, nk), 1) == nk - 1, jnp.concatenate([side, side], 1), pltpu.roll(row, nk - 1, 1)
        )
        for c, x in enumerate((row, moved)):
            for h in range(2):
                next_row(c, m, ni, h, x[:, 128 * h : 128 * h + 128])
    for q in range(nq):
        for h in range(2):
            carry = unit(ni - 1, q, h, *carry)
    c_sum, v_sum = carry

    def share(at, value):
        slot, group = stages[at]
        base = sum(len(stage[1]) + 1 for stage in stages[:at])
        sums[base + slot] = value
        for ids in group:
            pltpu.make_async_remote_copy(
                src_ref=sums.at[base + slot], dst_ref=sums.at[base + slot],
                send_sem=gsend.at[at], recv_sem=grecv.at[at],
                device_id=ids, device_id_type=MESH,
            ).start()

    def gather(at):
        size = len(stages[at][1])
        base = sum(len(stage[1]) + 1 for stage in stages[:at])
        every = sums.at[base : base + size]
        pltpu.make_async_copy(every, every, grecv.at[at]).wait()
        pltpu.make_async_copy(every, every, gsend.at[at]).wait()
        total = sums[base]
        for slot in range(1, size + 1):
            total = total + sums[base + slot]
        return total

    def fold(x):
        row = jnp.sum(x, axis=0, keepdims=True)
        row = row[:, :128] + row[:, 128:]
        return row + pltpu.roll(row, 64, 1)

    partial = jnp.where(iota((1, 128), 1) < 64, fold(c_sum), fold(v_sum))
    share(0, partial)
    face_swap(around, (1, 0, 0))

    zlo, zhi = pack(ni - 1, zsend[0], zsend[1])
    zsend[0] = zlo
    zsend[1] = zhi
    for step in AROUND:
        if step[1] or step[2]:
            face_swap(around, step)

    def spread_x(i):
        return 3.0 * wx[i + 2] + 2.0 * (wx[i + 1] + wx[i + 3]) + (wx[i] + wx[i + 4])

    def spread_z(xs):
        x = jnp.concatenate(xs, 0)
        high = x.astype(BF16)
        low = (x - high.astype(F32)).astype(BF16)
        both = jnp.dot(jnp.concatenate([high, low], 0), band[...], preferred_element_type=F32)
        return both[: x.shape[0]] + both[x.shape[0] :]

    def planes_xz(group):
        done = spread_z([spread_x(i) for i in group])
        for at, i in enumerate(group):
            for h in range(2):
                wy[i, h, 8 : 8 + nj, :] = done[nj * at : nj * at + nj, 128 * h : 128 * h + 128]

    for first in range(2, ni - 2, 4):
        planes_xz(range(first, min(first + 4, ni - 2)))
    for at in range(1, len(stages)):
        share(at, gather(at - 1))
    arrive(around)

    planes_xz((0, 1, ni - 2, ni - 1))
    lines = []
    for at in range(4):
        side, t = at >> 1, at & 1
        for p in range(2):
            rows_in[at, 6 + p : 7 + p, :] = corner_in[0, side, 2 * p + t : 2 * p + t + 1, :]
            rows_in[at, 8 + ni + p : 9 + ni + p, :] = corner_in[1, side, 2 * p + t : 2 * p + t + 1, :]
        x = [rows_in[at, 6 + d : 6 + d + ni, :] for d in range(5)]
        lines.append(3.0 * x[2] + 2.0 * (x[1] + x[3]) + (x[0] + x[4]))
    done = spread_z(lines)
    for at in range(4):
        yrow[at] = done[ni * at : ni * at + ni]

    wide = iota((nj + 16, 128), 1)
    even = lax.rem(lane, 2) == 0
    rims = []
    for side in range(2):
        x = jnp.where(
            wide < 4,
            pltpu.roll(rzz[side, 0], 128 - 2 * ni, 1),
            jnp.where(wide < 2 * ni + 4, rzz[side, 1], pltpu.roll(rzz[side, 2], 2 * ni, 1)),
        )
        x = (
            3.0 * x
            + 2.0 * (pltpu.roll(x, 2, 1) + pltpu.roll(x, 126, 1))
            + (pltpu.roll(x, 4, 1) + pltpu.roll(x, 124, 1))
        )
        rzs[side] = x
        y = [rzs[side, 6 + d : 6 + d + nj, :] for d in range(5)]
        y = 3.0 * y[2] + 2.0 * (y[1] + y[3]) + (y[0] + y[4])
        y = y + jnp.where(even, 0.0, 2.0 * pltpu.roll(y, 1, 1)) if side else (
            y + jnp.where(even, 2.0 * pltpu.roll(y, 127, 1), 0.0)
        )
        rims.append(y)

    for i in range(ni):
        for h in range(2):
            half = slice(128 * h, 128 * h + 128)
            for t in range(2):
                wy[i, h, 6 + t : 7 + t, :] = yrow[t, i : i + 1, half]
                wy[i, h, 8 + nj + t : 9 + nj + t, :] = yrow[2 + t, i : i + 1, half]
            y = [wy[i, h, 6 + d : 6 + d + nj, :] for d in range(5)]
            y = 3.0 * y[2] + 2.0 * (y[1] + y[3]) + (y[0] + y[4])
            if h:
                rim = jnp.where(lane >= 126, pltpu.roll(rims[1], 122 - 2 * i, 1), 0.0)
            else:
                rim = jnp.where(lane < 2, pltpu.roll(rims[0], 124 - 2 * i, 1), 0.0)
            out[i, :, half] = y + rim
    for copies in (beside, below, far, around):
        finish(copies)
    totals[...] = gather(len(stages) - 1)


def last_pass(cells, field, totals, out, comp, vol, ends, sem):
    copy = pltpu.make_async_copy(field, out, sem.at[0])
    copy.start()
    both = totals[...]
    first = iota((1, 128), 1) < 64
    ends[0] = jnp.sum(jnp.where(first, both, 0.0), axis=1, keepdims=True) / cells
    ends[1] = jnp.sum(jnp.where(first, 0.0, both), axis=1, keepdims=True) / cells
    small = [pltpu.make_async_copy(ends.at[at], dst, sem.at[1 + at]) for at, dst in enumerate((comp, vol))]
    for one in small:
        one.start()
    for one in small:
        one.wait()
    copy.wait()


def on_device(sizes, displacement, density, stiffness):
    ni, nj, nk = density.shape
    vmem = pl.BlockSpec(memory_space=pltpu.VMEM)
    hbm = pl.BlockSpec(memory_space=pltpu.HBM)
    everyone = sizes[0] * sizes[1] * sizes[2]
    members = everyone if everyone <= FEW else sizes[0] + sizes[1] * sizes[2]
    scratch = [
        displacement.shape, density.shape, stiffness.shape,
        (3, nj, nk), (3, ni, nk), (8, nk), (2, 2, nj, 128), (3, ni, nk), (8, nk), (nj, 128),
        (2, 3, ni + 1, 2, nj + 8, 128), (2, nj // 16, ni + 1, 8, nk), (2, 6, ni, 128), (2, 6, ni, 128), (nj, nk),
    ]
    later = [
        (ni + 4, nj, nk), (ni, 2, nj + 16, 128),
        (2, 2, ni, nk), (2, 2, 8, nk), (2, nj, 128), (4, ni + 16, nk), (2, 2, 8, nk),
        (2, 3, nj + 16, 128), (2, nj + 16, 128), (4, ni, nk), (members, 1, 128),
    ]
    field, totals = pl.pallas_call(
        functools.partial(kernel, sizes),
        out_shape=(
            jax.ShapeDtypeStruct((ni, nj, nk), F32),
            jax.ShapeDtypeStruct((1, 128), F32),
        ),
        in_specs=[hbm] * 3,
        out_specs=(vmem, vmem),
        scratch_shapes=[pltpu.VMEM(shape, F32) for shape in scratch]
        + [pltpu.VMEM((2, nj // 16, ni + 1, 48, nk), BF16), pltpu.VMEM((192, 256), BF16), pltpu.VMEM((nk, nk), BF16)]
        + [pltpu.VMEM(shape, F32) for shape in later]
        + [pltpu.SemaphoreType.DMA((count,)) for count in (4, 7, 7, 26, 26, 2, 2)]
        + [pltpu.SemaphoreType.REGULAR((1,))],
        compiler_params=pltpu.CompilerParams(
            collective_id=0, has_side_effects=True, vmem_limit_bytes=24 * 1024 * 1024
        ),
    )(*(pltpu.with_memory_space_constraint(x, pltpu.HBM) for x in (displacement, density, stiffness)))
    cells = float(ni * nj * nk * sizes[0] * sizes[1] * sizes[2])
    filtered, comp, vol = pl.pallas_call(
        functools.partial(last_pass, cells),
        out_shape=(
            jax.ShapeDtypeStruct((ni, nj, nk), F32),
            jax.ShapeDtypeStruct((1, 1), F32),
            jax.ShapeDtypeStruct((1, 1), F32),
        ),
        in_specs=[vmem] * 2,
        out_specs=(hbm, hbm, hbm),
        scratch_shapes=[pltpu.VMEM((2, 1, 1), F32), pltpu.SemaphoreType.DMA((3,))],
        compiler_params=pltpu.CompilerParams(vmem_limit_bytes=24 * 1024 * 1024),
    )(field, totals)
    return filtered, comp.reshape(()), vol.reshape(())


def solution(mesh):
    sizes = tuple(mesh.shape[axis] for axis in AXES)
    return jax.shard_map(
        functools.partial(on_device, sizes),
        mesh=mesh,
        in_specs=(P(None, "gx", "gy", "gz"), P("gx", "gy", "gz"), P()),
        out_specs=(P("gx", "gy", "gz"), P(), P()),
        check_vma=False,
    )
```

```python
import functools

import jax
import jax.numpy as jnp
from jax import lax
from jax.experimental import pallas as pl
from jax.experimental.pallas import tpu as pltpu
from jax.sharding import PartitionSpec as P

VOID = 0.001
H = (1.0, 2.0, 3.0, 2.0, 1.0)
MESH = pl.DeviceIdType.MESH
AXES = ("gx", "gy", "gz")
F32 = jnp.float32
BF16 = jnp.bfloat16
NODE_STEPS = [(a, b, c) for a in (0, 1) for b in (0, 1) for c in (0, 1) if a + b + c]
FEW = 64
AROUND = [(a, b, c) for a in (-1, 0, 1) for b in (-1, 0, 1) for c in (-1, 0, 1) if a or b or c]


def iota(shape, dim):
    return lax.broadcasted_iota(jnp.int32, shape, dim)


def line_sum(position, extent):
    total = None
    for d in range(5):
        at = position + (d - 2)
        term = jnp.where((at >= 0) & (at < extent), H[d], 0.0).astype(F32)
        total = term if total is None else total + term
    return total


def band_weights(stiff):
    rows, cols = 192, 128
    pick = jnp.where((iota((rows, 24), 0) >> 3) == iota((rows, 24), 1), 1.0, 0.0).astype(F32)

    def column(shape):
        col = iota(shape, 1)
        a, m, s = col >> 6, (col >> 4) & 3, col & 15
        edge = m == 3
        c = jnp.where(edge, jnp.where(s >= 3, 1, 0), s >> 3)
        m = jnp.where(edge, s - 3 * c, m)
        valid = jnp.logical_not(edge) | (s < 6)
        return 8 * m + 4 * a + c, valid, jnp.where(edge, 8, s & 7)

    total = None
    for b in (0, 1):
        q, valid, _ = column((24, cols))
        place = jnp.where((iota((24, cols), 0) == q + 2 * b) & valid, 1.0, 0.0).astype(F32)
        wide = jnp.dot(stiff, place, precision=lax.Precision.HIGHEST, preferred_element_type=F32)
        tall = jnp.dot(pick, wide, precision=lax.Precision.HIGHEST, preferred_element_type=F32)
        _, _, jj = column((rows, cols))
        term = jnp.where(jj - (iota((rows, cols), 0) & 7) == b, tall, 0.0)
        total = term if total is None else total + term
    high = total.astype(BF16)
    return jnp.concatenate([high, (total - high.astype(F32)).astype(BF16)], 1)


def kernel(
    sizes, u_hbm, rho_hbm, stiff_hbm, out, totals,
    u, rho, stiff, rx, ry, rxy, rz, ys, yd, zs,
    field, edge, line_f, line_u, inv, inv_x, parts, weights, band, wx, wy,
    ysend, corner_send, zsend, rows_in, corner_in, rzz, rzs, yrow,
    sums, insem, nsend, nrecv, fsend, frecv, gsend, grecv, known,
):
    ni, nj, nk = rho.shape
    n = dict(zip(AXES, sizes))
    me = {axis: lax.axis_index(axis) for axis in AXES}
    ny, nz = n["gy"], n["gz"]
    down = {axis: me[axis] > 0 for axis in AXES}
    up = {axis: me[axis] < n[axis] - 1 for axis in AXES}

    loads = []
    halves = [(u_hbm.at[:, :, :, at : at + 128], u.at[:, :, :, at : at + 128]) for at in (0, 128)]
    for at, (src, dst) in enumerate([(stiff_hbm, stiff)] + halves + [(rho_hbm, rho)]):
        copy = pltpu.make_async_copy(src, dst, insem.at[at])
        copy.start()
        loads.append(copy)

    def hop(step):
        ids, ok = {}, None
        for axis, s in zip(AXES, step):
            if s:
                ids[axis] = me[axis] + s
                flag = up[axis] if s > 0 else down[axis]
                ok = flag if ok is None else jnp.logical_and(ok, flag)
        return ids, ok

    def minus(step):
        return tuple(-s for s in step)

    everyone = n["gx"] * ny * nz
    mine = (me["gx"] * ny + me["gy"]) * nz + me["gz"]

    def place(at):
        at = jnp.int32(at)
        return {"gx": at // (ny * nz), "gy": lax.rem(at // nz, ny), "gz": lax.rem(at, nz)}

    line = [{"gx": lax.rem(me["gx"] + off, n["gx"])} for off in range(1, n["gx"])]
    sheet = [
        {"gy": lax.rem(me["gy"] + off // nz, ny), "gz": lax.rem(me["gz"] + off % nz, nz)}
        for off in range(1, ny * nz)
    ]
    if everyone <= FEW:
        others = [at + jnp.where(at >= mine, 1, 0) for at in range(everyone - 1)]
        stages = [(mine, [place(at) for at in others])]
    else:
        stages = [(me["gx"], line), (me["gy"] * nz + me["gz"], sheet)]
    lead = mine == everyone - 1

    def hear(semaphore, amount):
        @pl.when(amount > 0)
        def _():
            pl.semaphore_wait(semaphore, amount)

    barrier = pltpu.get_barrier_semaphore()
    beyond = [n[axis] - 1 - me[axis] > 1 for axis in AXES]
    beyond = jnp.logical_or(jnp.logical_or(beyond[0], beyond[1]), beyond[2])
    lower = 0
    for step in NODE_STEPS:
        ids, ok = hop(step)
        lower = lower + jnp.where(hop(minus(step))[1], 1, 0)

        @pl.when(ok)
        def _():
            pl.semaphore_signal(barrier, inc=1, device_id=ids, device_id_type=MESH)

    @pl.when(beyond)
    def _():
        pl.semaphore_signal(barrier, inc=1, device_id=place(everyone - 1), device_id_type=MESH)


    def node_route(step):
        a, b, c = step
        if c:
            return (zs.at[0:8], rz.at[a, b, 0:8]) if b else (zs, rz.at[a, b])
        if b:
            return (yd, rxy) if a else (ys, ry)
        return u.at[:, 0], rx

    def face_route(step):
        a, b, c = step
        hi_a, hi_b, hi_c = a > 0, b > 0, c > 0
        if c:
            rows = (slice(nj - 8, nj), slice(0, nj), slice(0, 8))[1 - b]
            to = (slice(0, 8), slice(8, 8 + nj), slice(8 + nj, 16 + nj))[1 - b]
            return zsend.at[int(hi_c), rows], rzz.at[1 - hi_c, 1 - a, to]
        if a and b:
            return corner_send.at[int(hi_a), int(hi_b)], corner_in.at[1 - hi_a, 1 - hi_b]
        if b:
            at = 2 * (1 - hi_b)
            return ysend.at[int(hi_b)], rows_in.at[at : at + 2, 8 : 8 + ni]
        return (wx.at[ni : ni + 2], wx.at[0:2]) if hi_a else (wx.at[2:4], wx.at[ni + 2 : ni + 4])

    def clear(missing, *refs):
        @pl.when(jnp.logical_not(missing))
        def _():
            for ref in refs:
                ref[...] = jnp.zeros(ref.shape, F32)


    def swap(copies, src, dst, send_sem, recv_sem, step):
        ids, sends = hop(step)
        copy = pltpu.make_async_remote_copy(
            src_ref=src, dst_ref=dst, send_sem=send_sem, recv_sem=recv_sem,
            device_id=ids, device_id_type=MESH,
        )
        copies.append((copy, sends, hop(minus(step))[1]))

        @pl.when(sends)
        def _():
            copy.start()

    def arrive(copies):
        for copy, _, takes in copies:

            @pl.when(takes)
            def _():
                copy.wait_recv()

    def finish(copies):
        for copy, sends, _ in copies:

            @pl.when(sends)
            def _():
                copy.wait_send()

    beside, below, far = [], [], []

    def node_swap(step):
        a, b, c = step
        at = NODE_STEPS.index(step)
        src, dst = node_route(step)
        copies = far if a else (below if b else beside)
        swap(copies, src, dst, nsend.at[at], nrecv.at[at], minus(step))

    def face_swap(copies, step):
        at = AROUND.index(step)
        src, dst = face_route(step)
        swap(copies, src, dst, fsend.at[at], frecv.at[at], step)

    loads[0].wait()
    weights[...] = band_weights(stiff[...])
    loads[1].wait()
    lane = iota((nj, 128), 1)
    packed = jnp.zeros((nj, 128), F32)
    for at in range(3 * ni):
        column = u[at // ni, at % ni, :, 0:128]
        packed = jnp.where(lane == at, pltpu.roll(column, at, 1) if at else column, packed)
    zs[...] = packed
    loads[2].wait()
    yd[...] = jnp.zeros(yd.shape, F32)
    for m in range(3):
        for i in range(ni):
            ys[m, i : i + 1, :] = u[m, i, 0:1, :]
        yd[m : m + 1, :] = u[m, 0, 0:1, :]
    hear(barrier, jnp.where(lead, everyone - 1, lower))
    for step in sorted(NODE_STEPS, key=lambda step: (sum(step), step)):
        node_swap(step)

    @pl.when(lead)
    def _():
        def greet(at, carry):
            pl.semaphore_signal(known.at[0], inc=1, device_id=place(at), device_id_type=MESH)
            return carry

        lax.fori_loop(0, everyone - 1, greet, 0)

    clear(up["gx"], rx, rxy, rz.at[1], wx.at[ni + 2 : ni + 4], corner_in.at[1], rzz.at[:, 2])
    clear(up["gy"], ry, rxy, rz.at[:, 1, 0:8], rows_in.at[2:4], corner_in.at[:, 1], rzz.at[:, :, 8 + nj : 16 + nj])
    clear(up["gz"], rz, rzz.at[1])
    clear(down["gx"], wx.at[0:2], corner_in.at[0], rzz.at[:, 0])
    clear(down["gy"], rows_in.at[0:2], corner_in.at[:, 0], rzz.at[:, :, 0:8])
    clear(down["gz"], rzz.at[0])
    apart = jnp.abs(iota((nk, nk), 0) - iota((nk, nk), 1))
    band[...] = jnp.maximum(3 - apart, 0).astype(F32).astype(BF16)
    edge[...] = jnp.zeros(edge.shape, F32)

    last = iota((nj, 128), 1) == 127
    nt = nj // 8

    def sharp(x):
        return x + (x - x.astype(BF16).astype(F32))

    def layer(h, to, at, source, col):
        for m in range(3):
            x = source(m, h)
            side = source(m, 1) if h == 0 else col
            turn = 127 if h == 0 else 127 - (m * ni + at)
            moved = jnp.where(last, pltpu.roll(side, turn, 1), pltpu.roll(x, 127, 1))
            for c, y in enumerate((x, moved)):
                field[c, m, to, h, 0:nj, :] = sharp(y)
                for jt in range(nt - 1):
                    edge[h, jt, to, 3 * c + m : 3 * c + m + 1, :] = y[8 * jt + 8 : 8 * jt + 9, :]
            for jt in range(nt):
                rows = slice(8 * jt, 8 * jt + 8)
                parts[h, jt, to, 16 * m : 16 * m + 16, :] = jnp.concatenate([x[rows], moved[rows]], 0).astype(BF16)

    def own(i):
        return lambda m, h: u[m, i, :, 128 * h : 128 * h + 128]

    def next_row(c, m, to, h, x):
        field[c, m, to, h, nj : nj + 1, :] = sharp(x)
        edge[h, nt - 1, to, 3 * c + m : 3 * c + m + 1, :] = x

    def own_row(i, carry):
        at = pl.ds(i, 1)
        for h in range(2):
            for cm in range(6):
                field[cm // 3, cm % 3, i, h, nj : nj + 1, :] = line_f[h, cm, at, :]
                edge[h, nt - 1, i, cm : cm + 1, :] = line_u[h, cm, at, :]
        return carry

    none8 = jnp.zeros((8, nk), F32)

    def both(take, tiles):
        return jnp.concatenate([take(*tile) for tile in tiles], 1)

    def unit(tiles, carry):
        c_sum, v_sum = carry
        data = []
        for a in range(2):
            data.append(both(lambda i, jt, h: parts[h, jt, i + a], tiles))
            rim = both(lambda i, jt, h: edge[h, jt, i + a], tiles)
            data.append(jnp.concatenate([rim, none8], 0).astype(BF16))
        product = jnp.dot(weights[...], jnp.concatenate(data + data, 0), preferred_element_type=F32)
        energy = None
        for r in range(24):
            m, a, b, c = r >> 3, (r >> 2) & 1, (r >> 1) & 1, r & 1
            f = both(lambda i, jt, h: field[c, m, i + a, h, 8 * jt + b : 8 * jt + b + 8, :], tiles)
            term = product[8 * r : 8 * r + 8] * f
            energy = term if energy is None else energy + term

        d = both(lambda i, jt, h: rho[i, 8 * jt : 8 * jt + 8, 128 * h : 128 * h + 128], tiles)
        scale = both(
            lambda i, jt, h: inv[8 * jt : 8 * jt + 8, 128 * h : 128 * h + 128] * inv_x[pl.ds(i, 1), :], tiles
        )
        w = (-3.0 * (1.0 - VOID)) * d * d * energy * scale
        for t, (i, jt, h) in enumerate(tiles):
            wx[i + 2, 8 * jt : 8 * jt + 8, 128 * h : 128 * h + 128] = w[:, 128 * t : 128 * t + 128]
        return c_sum + (VOID + d * d * d * (1.0 - VOID)) * energy, v_sum + d

    def sweep(h):
        def body(t, carry):
            for step in (1, 2):
                layer(h, 2 * t + step, 2 * t + step, own(2 * t + step), rz[0, 0])
            for jt in range(nt - 1):
                carry = unit([(2 * t, jt, h), (2 * t + 1, jt, h)], carry)
            return carry

        return body

    def rest(h, carry):
        layer(h, ni - 1, ni - 1, own(ni - 1), rz[0, 0])
        todo = [(ni - 2, jt, h) for jt in range(nt - 1)]
        if h:
            todo += [(ni - 2, jt, 0) for jt in range((nt - 1) // 2 * 2, nt - 1)]
        for at in range(0, len(todo) // 2 * 2, 2):
            carry = unit(todo[at : at + 2], carry)
        return carry

    line_x = line_sum(me["gx"] * ni + iota((ni, 128), 0), n["gx"] * ni)
    inv_x[...] = 1.0 / line_x
    loads[3].wait()
    inv[...] = 1.0 / (
        line_sum(me["gy"] * nj + iota((nj, nk), 0), ny * nj)
        * line_sum(me["gz"] * nk + iota((nj, nk), 1), nz * nk)
    )
    carry = (none8, none8)
    layer(0, 0, 0, own(0), None)
    carry = lax.fori_loop(0, ni // 2 - 1, sweep(0), carry, unroll=7)
    carry = rest(0, carry)
    arrive(beside)
    layer(1, 0, 0, own(0), rz[0, 0])
    carry = lax.fori_loop(0, ni // 2 - 1, sweep(1), carry, unroll=7)
    carry = rest(1, carry)
    arrive(below)

    def row_pair(h):
        for m in range(3):
            base = ry[m]
            if h:
                mine = iota((ni, 128), 1) == iota((ni, 128), 0) + m * ni
                side = jnp.sum(jnp.where(mine, rz[0, 1, 0:1, :], 0.0), axis=1, keepdims=True)
            else:
                side = pltpu.roll(base[:, 128:256], 127, 1)
            x = base[:, 128 * h : 128 * h + 128]
            moved = jnp.where(iota((ni, 128), 1) == 127, side, pltpu.roll(x, 127, 1))
            for c, y in enumerate((x, moved)):
                line_u[h, 3 * c + m] = y
                line_f[h, 3 * c + m] = sharp(y)

    def upper(i, carry):
        return unit([(i, nt - 1, 0), (i, nt - 1, 1)], carry)

    for h in range(2):
        row_pair(h)
    lax.fori_loop(0, ni, own_row, 0, unroll=4)
    carry = lax.fori_loop(0, ni - 1, upper, carry, unroll=ni - 1)
    zlo = zhi = jnp.zeros((nj, 128), F32)

    def pack(i, zlo, zhi):
        slot = (lane >> 1) == i + 2
        plane = wx[i + 2]
        zlo = jnp.where(slot, pltpu.roll(plane[:, 0:128], 2 * i + 4, 1), zlo)
        zhi = jnp.where(slot, pltpu.roll(plane[:, nk - 128 : nk], (2 * i + 6) % 128, 1), zhi)
        for t in range(2):
            for top, row in enumerate((t, nj - 2 + t)):
                line_at = wx[i + 2, row : row + 1, :]
                ysend[top, t, i : i + 1, :] = line_at
                if i < 2 or i >= ni - 2:
                    p = i if i < 2 else i - ni + 2
                    corner_send[int(i >= 2), top, 2 * p + t : 2 * p + t + 1, :] = line_at
        return zlo, zhi

    for i in range(ni - 1):
        zlo, zhi = pack(i, zlo, zhi)
    zsend[0] = zlo
    zsend[1] = zhi
    hear(known.at[0], jnp.where(lead, 0, 1))
    around = []
    face_swap(around, (-1, 0, 0))
    arrive(far)
    for h in range(2):
        layer(h, ni, 0, lambda m, h: rx[m, :, 128 * h : 128 * h + 128], rz[1, 0])
    for m in range(3):
        row = rxy[m : m + 1, :]
        side = pltpu.roll(rz[1, 1, 0:1, :], 127 - m * ni, 1)
        moved = jnp.where(
            iota((1, nk), 1) == nk - 1, jnp.concatenate([side, side], 1), pltpu.roll(row, nk - 1, 1)
        )
        for c, x in enumerate((row, moved)):
            for h in range(2):
                next_row(c, m, ni, h, x[:, 128 * h : 128 * h + 128])
    for jt in range(nt):
        carry = unit([(ni - 1, jt, 0), (ni - 1, jt, 1)], carry)
    c_sum, v_sum = carry

    def share(at, value):
        slot, group = stages[at]
        base = sum(len(stage[1]) + 1 for stage in stages[:at])
        sums[base + slot] = value
        for ids in group:
            pltpu.make_async_remote_copy(
                src_ref=sums.at[base + slot], dst_ref=sums.at[base + slot],
                send_sem=gsend.at[at], recv_sem=grecv.at[at],
                device_id=ids, device_id_type=MESH,
            ).start()

    def gather(at):
        size = len(stages[at][1])
        base = sum(len(stage[1]) + 1 for stage in stages[:at])
        every = sums.at[base : base + size]
        pltpu.make_async_copy(every, every, grecv.at[at]).wait()
        pltpu.make_async_copy(every, every, gsend.at[at]).wait()
        total = sums[base]
        for slot in range(1, size + 1):
            total = total + sums[base + slot]
        return total

    def fold(x):
        row = jnp.sum(x, axis=0, keepdims=True)
        row = row[:, :128] + row[:, 128:]
        return row + pltpu.roll(row, 64, 1)

    partial = jnp.where(iota((1, 128), 1) < 64, fold(c_sum), fold(v_sum))
    share(0, partial)
    face_swap(around, (1, 0, 0))

    zlo, zhi = pack(ni - 1, zsend[0], zsend[1])
    zsend[0] = zlo
    zsend[1] = zhi
    for step in AROUND:
        if step[1] or step[2]:
            face_swap(around, step)

    def spread_x(i):
        return 3.0 * wx[i + 2] + 2.0 * (wx[i + 1] + wx[i + 3]) + (wx[i] + wx[i + 4])

    def spread_z(xs):
        x = jnp.concatenate(xs, 0)
        high = x.astype(BF16)
        low = (x - high.astype(F32)).astype(BF16)
        both = jnp.dot(jnp.concatenate([high, low], 0), band[...], preferred_element_type=F32)
        return both[: x.shape[0]] + both[x.shape[0] :]

    def planes_xz(group):
        done = spread_z([spread_x(i) for i in group])
        for at, i in enumerate(group):
            for h in range(2):
                wy[i, h, 8 : 8 + nj, :] = done[nj * at : nj * at + nj, 128 * h : 128 * h + 128]

    for first in range(2, ni - 2, 4):
        planes_xz(range(first, min(first + 4, ni - 2)))
    for at in range(1, len(stages)):
        share(at, gather(at - 1))
    arrive(around)

    planes_xz((0, 1, ni - 2, ni - 1))
    lines = []
    for at in range(4):
        side, t = at >> 1, at & 1
        for p in range(2):
            rows_in[at, 6 + p : 7 + p, :] = corner_in[0, side, 2 * p + t : 2 * p + t + 1, :]
            rows_in[at, 8 + ni + p : 9 + ni + p, :] = corner_in[1, side, 2 * p + t : 2 * p + t + 1, :]
        x = [rows_in[at, 6 + d : 6 + d + ni, :] for d in range(5)]
        lines.append(3.0 * x[2] + 2.0 * (x[1] + x[3]) + (x[0] + x[4]))
    done = spread_z(lines)
    for at in range(4):
        yrow[at] = done[ni * at : ni * at + ni]

    wide = iota((nj + 16, 128), 1)
    even = lax.rem(lane, 2) == 0
    rims = []
    for side in range(2):
        x = jnp.where(
            wide < 4,
            pltpu.roll(rzz[side, 0], 128 - 2 * ni, 1),
            jnp.where(wide < 2 * ni + 4, rzz[side, 1], pltpu.roll(rzz[side, 2], 2 * ni, 1)),
        )
        x = (
            3.0 * x
            + 2.0 * (pltpu.roll(x, 2, 1) + pltpu.roll(x, 126, 1))
            + (pltpu.roll(x, 4, 1) + pltpu.roll(x, 124, 1))
        )
        rzs[side] = x
        y = [rzs[side, 6 + d : 6 + d + nj, :] for d in range(5)]
        y = 3.0 * y[2] + 2.0 * (y[1] + y[3]) + (y[0] + y[4])
        y = y + jnp.where(even, 0.0, 2.0 * pltpu.roll(y, 1, 1)) if side else (
            y + jnp.where(even, 2.0 * pltpu.roll(y, 127, 1), 0.0)
        )
        rims.append(y)

    for i in range(ni):
        for h in range(2):
            half = slice(128 * h, 128 * h + 128)
            for t in range(2):
                wy[i, h, 6 + t : 7 + t, :] = yrow[t, i : i + 1, half]
                wy[i, h, 8 + nj + t : 9 + nj + t, :] = yrow[2 + t, i : i + 1, half]
            y = [wy[i, h, 6 + d : 6 + d + nj, :] for d in range(5)]
            y = 3.0 * y[2] + 2.0 * (y[1] + y[3]) + (y[0] + y[4])
            if h:
                rim = jnp.where(lane >= 126, pltpu.roll(rims[1], 122 - 2 * i, 1), 0.0)
            else:
                rim = jnp.where(lane < 2, pltpu.roll(rims[0], 124 - 2 * i, 1), 0.0)
            out[i, :, half] = y + rim
    for copies in (beside, below, far, around):
        finish(copies)
    totals[...] = gather(len(stages) - 1)


def last_pass(cells, field, totals, out, comp, vol, ends, sem):
    copy = pltpu.make_async_copy(field, out, sem.at[0])
    copy.start()
    both = totals[...]
    first = iota((1, 128), 1) < 64
    ends[0] = jnp.sum(jnp.where(first, both, 0.0), axis=1, keepdims=True) / cells
    ends[1] = jnp.sum(jnp.where(first, 0.0, both), axis=1, keepdims=True) / cells
    small = [pltpu.make_async_copy(ends.at[at], dst, sem.at[1 + at]) for at, dst in enumerate((comp, vol))]
    for one in small:
        one.start()
    for one in small:
        one.wait()
    copy.wait()


def on_device(sizes, displacement, density, stiffness):
    ni, nj, nk = density.shape
    vmem = pl.BlockSpec(memory_space=pltpu.VMEM)
    hbm = pl.BlockSpec(memory_space=pltpu.HBM)
    everyone = sizes[0] * sizes[1] * sizes[2]
    members = everyone if everyone <= FEW else sizes[0] + sizes[1] * sizes[2]
    scratch = [
        displacement.shape, density.shape, stiffness.shape,
        (3, nj, nk), (3, ni, nk), (8, nk), (2, 2, nj, 128), (3, ni, nk), (8, nk), (nj, 128),
        (2, 3, ni + 1, 2, nj + 8, 128), (2, nj // 8, ni + 1, 8, 128), (2, 6, ni, 128), (2, 6, ni, 128), (nj, nk), (ni, 128),
    ]
    later = [
        (ni + 4, nj, nk), (ni, 2, nj + 16, 128),
        (2, 2, ni, nk), (2, 2, 8, nk), (2, nj, 128), (4, ni + 16, nk), (2, 2, 8, nk),
        (2, 3, nj + 16, 128), (2, nj + 16, 128), (4, ni, nk), (members, 1, 128),
    ]
    field, totals = pl.pallas_call(
        functools.partial(kernel, sizes),
        out_shape=(
            jax.ShapeDtypeStruct((ni, nj, nk), F32),
            jax.ShapeDtypeStruct((1, 128), F32),
        ),
        in_specs=[hbm] * 3,
        out_specs=(vmem, vmem),
        scratch_shapes=[pltpu.VMEM(shape, F32) for shape in scratch]
        + [pltpu.VMEM((2, nj // 8, ni + 1, 48, 128), BF16), pltpu.VMEM((192, 256), BF16), pltpu.VMEM((nk, nk), BF16)]
        + [pltpu.VMEM(shape, F32) for shape in later]
        + [pltpu.SemaphoreType.DMA((count,)) for count in (4, 7, 7, 26, 26, 2, 2)]
        + [pltpu.SemaphoreType.REGULAR((1,))],
        compiler_params=pltpu.CompilerParams(
            collective_id=0, has_side_effects=True, vmem_limit_bytes=24 * 1024 * 1024
        ),
    )(*(pltpu.with_memory_space_constraint(x, pltpu.HBM) for x in (displacement, density, stiffness)))
    cells = float(ni * nj * nk * sizes[0] * sizes[1] * sizes[2])
    filtered, comp, vol = pl.pallas_call(
        functools.partial(last_pass, cells),
        out_shape=(
            jax.ShapeDtypeStruct((ni, nj, nk), F32),
            jax.ShapeDtypeStruct((1, 1), F32),
            jax.ShapeDtypeStruct((1, 1), F32),
        ),
        in_specs=[vmem] * 2,
        out_specs=(hbm, hbm, hbm),
        scratch_shapes=[pltpu.VMEM((2, 1, 1), F32), pltpu.SemaphoreType.DMA((3,))],
        compiler_params=pltpu.CompilerParams(vmem_limit_bytes=24 * 1024 * 1024),
    )(field, totals)
    return filtered, comp.reshape(()), vol.reshape(())


def solution(mesh):
    sizes = tuple(mesh.shape[axis] for axis in AXES)
    return jax.shard_map(
        functools.partial(on_device, sizes),
        mesh=mesh,
        in_specs=(P(None, "gx", "gy", "gz"), P("gx", "gy", "gz"), P()),
        out_specs=(P("gx", "gy", "gz"), P(), P()),
        check_vma=False,
    )
```

```python
import functools
import itertools
import math

import jax
import jax.numpy as jnp
from jax import lax
from jax.experimental import pallas as pl
from jax.experimental.pallas import tpu as pltpu
from jax.sharding import PartitionSpec as P

VOID = 0.001
H = (1.0, 2.0, 3.0, 2.0, 1.0)
MESH = pl.DeviceIdType.MESH
AXES = ("gx", "gy", "gz")
F32 = jnp.float32
BF16 = jnp.bfloat16
NODE_STEPS = [(a, b, c) for a in (0, 1) for b in (0, 1) for c in (0, 1) if a + b + c]
FEW = 64
CHUNKS = 4
AROUND = [(a, b, c) for a in (-1, 0, 1) for b in (-1, 0, 1) for c in (-1, 0, 1) if a or b or c]


def iota(shape, dim):
    return lax.broadcasted_iota(jnp.int32, shape, dim)


def line_sum(position, extent):
    total = None
    for d in range(5):
        at = position + (d - 2)
        term = jnp.where((at >= 0) & (at < extent), H[d], 0.0).astype(F32)
        total = term if total is None else total + term
    return total


def band_weights(stiff):
    rows, cols = 192, 128
    pick = jnp.where((iota((rows, 24), 0) >> 3) == iota((rows, 24), 1), 1.0, 0.0).astype(F32)

    def column(shape):
        col = iota(shape, 1)
        a, m, s = col >> 6, (col >> 4) & 3, col & 15
        edge = m == 3
        c = jnp.where(edge, jnp.where(s >= 3, 1, 0), s >> 3)
        m = jnp.where(edge, s - 3 * c, m)
        valid = jnp.logical_not(edge) | (s < 6)
        return 8 * m + 4 * a + c, valid, jnp.where(edge, 8, s & 7)

    total = None
    for b in (0, 1):
        q, valid, _ = column((24, cols))
        place = jnp.where((iota((24, cols), 0) == q + 2 * b) & valid, 1.0, 0.0).astype(F32)
        wide = jnp.dot(stiff, place, precision=lax.Precision.HIGHEST, preferred_element_type=F32)
        tall = jnp.dot(pick, wide, precision=lax.Precision.HIGHEST, preferred_element_type=F32)
        _, _, jj = column((rows, cols))
        term = jnp.where(jj - (iota((rows, cols), 0) & 7) == b, tall, 0.0)
        total = term if total is None else total + term
    high = total.astype(BF16)
    return jnp.concatenate([high, (total - high.astype(F32)).astype(BF16)], 1)


def kernel(
    sizes, u_hbm, rho_hbm, stiff_hbm, out, totals,
    u, rho, stiff, rx, ry, rxy, rz, ys, yd, zs,
    field, edge, line_f, line_u, inv, inv_x, parts, weights, band, wx, wy,
    ysend, corner_send, zsend, rows_in, corner_in, rzz, rzs, yrow, tally,
    sums, insem, nsend, nrecv, fsend, frecv, gsend, grecv, known,
):
    ni, nj, nk = rho.shape
    n = dict(zip(AXES, sizes))
    me = {axis: lax.axis_index(axis) for axis in AXES}
    ny, nz = n["gy"], n["gz"]
    down = {axis: me[axis] > 0 for axis in AXES}
    up = {axis: me[axis] < n[axis] - 1 for axis in AXES}

    loads = []
    halves = [(u_hbm.at[:, 1:, :, at : at + 128], u.at[:, 1:, :, at : at + 128]) for at in (0, 128)]
    first = [(u_hbm.at[:, 0], u.at[:, 0]), (stiff_hbm, stiff)]
    for at, (src, dst) in enumerate(first + halves + [(rho_hbm, rho)]):
        copy = pltpu.make_async_copy(src, dst, insem.at[at])
        copy.start()
        loads.append(copy)

    def hop(step):
        ids, ok = {}, None
        for axis, s in zip(AXES, step):
            if s:
                ids[axis] = me[axis] + s
                flag = up[axis] if s > 0 else down[axis]
                ok = flag if ok is None else jnp.logical_and(ok, flag)
        return ids, ok

    def minus(step):
        return tuple(-s for s in step)

    everyone = n["gx"] * ny * nz
    mine = (me["gx"] * ny + me["gy"]) * nz + me["gz"]

    def place(at):
        at = jnp.int32(at)
        return {"gx": at // (ny * nz), "gy": lax.rem(at // nz, ny), "gz": lax.rem(at, nz)}

    line = [{"gx": lax.rem(me["gx"] + off, n["gx"])} for off in range(1, n["gx"])]
    sheet = [
        {"gy": lax.rem(me["gy"] + off // nz, ny), "gz": lax.rem(me["gz"] + off % nz, nz)}
        for off in range(1, ny * nz)
    ]
    if everyone <= FEW:
        others = [at + jnp.where(at >= mine, 1, 0) for at in range(everyone - 1)]
        stages = [(mine, [place(at) for at in others])]
    else:
        stages = [(me["gx"], line), (me["gy"] * nz + me["gz"], sheet)]
    lead = mine == everyone - 1

    def hear(semaphore, amount):
        @pl.when(amount > 0)
        def _():
            pl.semaphore_wait(semaphore, amount)

    barrier = pltpu.get_barrier_semaphore()
    beyond = [n[axis] - 1 - me[axis] > 1 for axis in AXES]
    beyond = jnp.logical_or(jnp.logical_or(beyond[0], beyond[1]), beyond[2])
    lower = 0
    for step in NODE_STEPS:
        ids, ok = hop(step)
        lower = lower + jnp.where(hop(minus(step))[1], 1, 0)

        @pl.when(ok)
        def _():
            pl.semaphore_signal(barrier, inc=1, device_id=ids, device_id_type=MESH)

    @pl.when(beyond)
    def _():
        pl.semaphore_signal(barrier, inc=1, device_id=place(everyone - 1), device_id_type=MESH)


    def node_route(step):
        a, b, c = step
        if c:
            return (zs.at[0:8], rz.at[a, b, 0:8]) if b else (zs, rz.at[a, b])
        if b:
            return (yd, rxy) if a else (ys, ry)
        return u.at[:, 0], rx

    def face_route(step):
        a, b, c = step
        hi_a, hi_b, hi_c = a > 0, b > 0, c > 0
        if c:
            rows = (slice(nj - 8, nj), slice(0, nj), slice(0, 8))[1 - b]
            to = (slice(0, 8), slice(8, 8 + nj), slice(8 + nj, 16 + nj))[1 - b]
            return zsend.at[int(hi_c), rows], rzz.at[1 - hi_c, 1 - a, to]
        if a and b:
            return corner_send.at[int(hi_a), int(hi_b)], corner_in.at[1 - hi_a, 1 - hi_b]
        if b:
            at = 2 * (1 - hi_b)
            return ysend.at[int(hi_b)], rows_in.at[at : at + 2, 8 : 8 + ni]
        return (wx.at[ni : ni + 2], wx.at[0:2]) if hi_a else (wx.at[2:4], wx.at[ni + 2 : ni + 4])

    def clear(missing, *refs):
        @pl.when(jnp.logical_not(missing))
        def _():
            for ref in refs:
                ref[...] = jnp.zeros(ref.shape, F32)


    def swap(src, dst, send_sem, recv_sem, step):
        ids, sends = hop(step)

        @pl.when(sends)
        def _():
            pltpu.make_async_remote_copy(
                src_ref=src, dst_ref=dst, send_sem=send_sem, recv_sem=recv_sem,
                device_id=ids, device_id_type=MESH,
            ).start()

    def states(axis):
        if n[axis] == 1:
            return [((), True)]
        low, high = down[axis], up[axis]
        found = [((1,), jnp.logical_not(low)), ((-1,), jnp.logical_not(high))]
        return found + ([((-1, 1), jnp.logical_and(low, high))] if n[axis] > 2 else [])

    def drain(semaphore, items):
        for case in itertools.product(*(states(axis) for axis in AXES)):
            rows = sum(
                math.prod(shape) // 128
                for step, shape in items
                if all(s == 0 or s in ways for s, (ways, _) in zip(step, case))
            )
            if rows:
                flag = jnp.logical_and(jnp.logical_and(case[0][1], case[1][1]), case[2][1])

                @pl.when(flag)
                def _():
                    pltpu.make_async_copy(tally.at[0:rows], tally.at[0:rows], semaphore).wait()

    def node_items(steps, sign):
        return [(tuple(sign * s for s in step), node_route(step)[1].shape) for step in steps]

    def face_items(sign):
        return [(tuple(sign * s for s in step), face_route(step)[1].shape) for step in AROUND]

    def group_of(step):
        return 2 if step[0] else (1 if step[1] else 0)

    def node_swap(step):
        src, dst = node_route(step)
        swap(src, dst, nsend.at[0], nrecv.at[group_of(step)], minus(step))

    def arrive(which):
        drain(nrecv.at[which], node_items([s for s in NODE_STEPS if group_of(s) == which], 1))

    def face_swap(step):
        src, dst = face_route(step)
        swap(src, dst, fsend.at[0], frecv.at[0], step)

    loads[0].wait()
    hear(barrier, jnp.where(lead, everyone - 1, lower))
    node_swap((1, 0, 0))

    @pl.when(lead)
    def _():
        def greet(at, carry):
            pl.semaphore_signal(known.at[0], inc=1, device_id=place(at), device_id_type=MESH)
            return carry

        lax.fori_loop(0, everyone - 1, greet, 0)

    loads[2].wait()
    lane = iota((nj, 128), 1)
    packed = [jnp.zeros((nj, 128), F32)] * 6
    for at in range(3 * ni):
        column = u[at // ni, at % ni, :, 0:128]
        packed[at % 6] = jnp.where(lane == at, pltpu.roll(column, at, 1) if at else column, packed[at % 6])
    zs[...] = (packed[0] + packed[1]) + (packed[2] + packed[3]) + (packed[4] + packed[5])
    loads[3].wait()
    yd[...] = jnp.zeros(yd.shape, F32)
    for m in range(3):
        for i in range(ni):
            ys[m, i : i + 1, :] = u[m, i, 0:1, :]
        yd[m : m + 1, :] = u[m, 0, 0:1, :]
    for step in sorted(NODE_STEPS, key=lambda step: (sum(step), step)):
        if step != (1, 0, 0):
            node_swap(step)
    loads[1].wait()
    weights[...] = band_weights(stiff[...])
    clear(up["gx"], rx, rxy, rz.at[1], wx.at[ni + 2 : ni + 4], corner_in.at[1], rzz.at[:, 2])
    clear(up["gy"], ry, rxy, rz.at[:, 1, 0:8], rows_in.at[2:4], corner_in.at[:, 1], rzz.at[:, :, 8 + nj : 16 + nj])
    clear(up["gz"], rz, rzz.at[1])
    clear(down["gx"], wx.at[0:2], corner_in.at[0], rzz.at[:, 0])
    clear(down["gy"], rows_in.at[0:2], corner_in.at[:, 0], rzz.at[:, :, 0:8])
    clear(down["gz"], rzz.at[0])
    apart = jnp.abs(iota((nk, nk), 0) - iota((nk, nk), 1))
    band[...] = jnp.maximum(3 - apart, 0).astype(F32).astype(BF16)
    edge[...] = jnp.zeros(edge.shape, F32)

    last = iota((nj, 128), 1) == 127
    nt = nj // 8

    def sharp(x):
        return x + (x - x.astype(BF16).astype(F32))

    def layer(h, to, at, source, col):
        for m in range(3):
            x = source(m, h)
            side = source(m, 1) if h == 0 else col
            turn = 127 if h == 0 else 127 - (m * ni + at)
            moved = jnp.where(last, pltpu.roll(side, turn, 1), pltpu.roll(x, 127, 1))
            for c, y in enumerate((x, moved)):
                field[c, m, to, h, 0:nj, :] = sharp(y)
                for jt in range(nt - 1):
                    edge[h, jt, to, 3 * c + m : 3 * c + m + 1, :] = y[8 * jt + 8 : 8 * jt + 9, :]
            for jt in range(nt):
                rows = slice(8 * jt, 8 * jt + 8)
                parts[h, jt, to, 16 * m : 16 * m + 16, :] = jnp.concatenate([x[rows], moved[rows]], 0).astype(BF16)

    def own(i):
        return lambda m, h: u[m, i, :, 128 * h : 128 * h + 128]

    def next_row(c, m, to, h, x):
        field[c, m, to, h, nj : nj + 1, :] = sharp(x)
        edge[h, nt - 1, to, 3 * c + m : 3 * c + m + 1, :] = x

    def own_row(i, carry):
        at = pl.ds(i, 1)
        for h in range(2):
            for cm in range(6):
                field[cm // 3, cm % 3, i, h, nj : nj + 1, :] = line_f[h, cm, at, :]
                edge[h, nt - 1, i, cm : cm + 1, :] = line_u[h, cm, at, :]
        return carry

    none8 = jnp.zeros((8, nk), F32)

    def both(take, tiles):
        return jnp.concatenate([take(*tile) for tile in tiles], 1)

    def unit(tiles, carry):
        c_sum, v_sum = carry
        data = []
        for a in range(2):
            data.append(both(lambda i, jt, h: parts[h, jt, i + a], tiles))
            rim = both(lambda i, jt, h: edge[h, jt, i + a], tiles)
            data.append(jnp.concatenate([rim, none8], 0).astype(BF16))
        product = jnp.dot(weights[...], jnp.concatenate(data + data, 0), preferred_element_type=F32)
        energy = None
        for r in range(24):
            m, a, b, c = r >> 3, (r >> 2) & 1, (r >> 1) & 1, r & 1
            f = both(lambda i, jt, h: field[c, m, i + a, h, 8 * jt + b : 8 * jt + b + 8, :], tiles)
            term = product[8 * r : 8 * r + 8] * f
            energy = term if energy is None else energy + term

        d = both(lambda i, jt, h: rho[i, 8 * jt : 8 * jt + 8, 128 * h : 128 * h + 128], tiles)
        scale = both(
            lambda i, jt, h: inv[8 * jt : 8 * jt + 8, 128 * h : 128 * h + 128] * inv_x[pl.ds(i, 1), :], tiles
        )
        w = (-3.0 * (1.0 - VOID)) * d * d * energy * scale
        for t, (i, jt, h) in enumerate(tiles):
            wx[i + 2, 8 * jt : 8 * jt + 8, 128 * h : 128 * h + 128] = w[:, 128 * t : 128 * t + 128]
        return c_sum + (VOID + d * d * d * (1.0 - VOID)) * energy, v_sum + d

    def sweep(h):
        def body(t, carry):
            for step in (1, 2):
                layer(h, 2 * t + step, 2 * t + step, own(2 * t + step), rz[0, 0])
            for jt in range(nt - 1):
                carry = unit([(2 * t, jt, h), (2 * t + 1, jt, h)], carry)
            return carry

        return body

    def rest(h, carry):
        layer(h, ni - 1, ni - 1, own(ni - 1), rz[0, 0])
        todo = [(ni - 2, jt, h) for jt in range(nt - 1)]
        if h:
            todo += [(ni - 2, jt, 0) for jt in range((nt - 1) // 2 * 2, nt - 1)]
        for at in range(0, len(todo) // 2 * 2, 2):
            carry = unit(todo[at : at + 2], carry)
        return carry

    line_x = line_sum(me["gx"] * ni + iota((ni, 128), 0), n["gx"] * ni)
    inv_x[...] = 1.0 / line_x
    loads[4].wait()
    inv[...] = 1.0 / (
        line_sum(me["gy"] * nj + iota((nj, nk), 0), ny * nj)
        * line_sum(me["gz"] * nk + iota((nj, nk), 1), nz * nk)
    )
    carry = (none8, none8)
    layer(0, 0, 0, own(0), None)
    carry = lax.fori_loop(0, ni // 2 - 1, sweep(0), carry, unroll=7)
    carry = rest(0, carry)
    arrive(0)
    layer(1, 0, 0, own(0), rz[0, 0])
    carry = lax.fori_loop(0, ni // 2 - 1, sweep(1), carry, unroll=7)
    carry = rest(1, carry)
    arrive(1)

    def row_pair(h):
        for m in range(3):
            base = ry[m]
            if h:
                mine = iota((ni, 128), 1) == iota((ni, 128), 0) + m * ni
                side = jnp.sum(jnp.where(mine, rz[0, 1, 0:1, :], 0.0), axis=1, keepdims=True)
            else:
                side = pltpu.roll(base[:, 128:256], 127, 1)
            x = base[:, 128 * h : 128 * h + 128]
            moved = jnp.where(iota((ni, 128), 1) == 127, side, pltpu.roll(x, 127, 1))
            for c, y in enumerate((x, moved)):
                line_u[h, 3 * c + m] = y
                line_f[h, 3 * c + m] = sharp(y)

    def upper(i, carry):
        return unit([(i, nt - 1, 0), (i, nt - 1, 1)], carry)

    for h in range(2):
        row_pair(h)
    lax.fori_loop(0, ni, own_row, 0, unroll=ni)
    carry = lax.fori_loop(0, ni - 1, upper, carry, unroll=ni - 1)
    zlo = zhi = jnp.zeros((nj, 128), F32)

    def pack(i, zlo, zhi):
        slot = (lane >> 1) == i + 2
        plane = wx[i + 2]
        zlo = jnp.where(slot, pltpu.roll(plane[:, 0:128], 2 * i + 4, 1), zlo)
        zhi = jnp.where(slot, pltpu.roll(plane[:, nk - 128 : nk], (2 * i + 6) % 128, 1), zhi)
        for t in range(2):
            for top, row in enumerate((t, nj - 2 + t)):
                line_at = wx[i + 2, row : row + 1, :]
                ysend[top, t, i : i + 1, :] = line_at
                if i < 2 or i >= ni - 2:
                    p = i if i < 2 else i - ni + 2
                    corner_send[int(i >= 2), top, 2 * p + t : 2 * p + t + 1, :] = line_at
        return zlo, zhi

    for i in range(ni - 1):
        zlo, zhi = pack(i, zlo, zhi)
    zsend[0] = zlo
    zsend[1] = zhi
    hear(known.at[0], jnp.where(lead, 0, 1))
    arrive(2)
    for h in range(2):
        layer(h, ni, 0, lambda m, h: rx[m, :, 128 * h : 128 * h + 128], rz[1, 0])
    for m in range(3):
        row = rxy[m : m + 1, :]
        side = pltpu.roll(rz[1, 1, 0:1, :], 127 - m * ni, 1)
        moved = jnp.where(
            iota((1, nk), 1) == nk - 1, jnp.concatenate([side, side], 1), pltpu.roll(row, nk - 1, 1)
        )
        for c, x in enumerate((row, moved)):
            for h in range(2):
                next_row(c, m, ni, h, x[:, 128 * h : 128 * h + 128])
    for jt in range(nt):
        carry = unit([(ni - 1, jt, 0), (ni - 1, jt, 1)], carry)
    c_sum, v_sum = carry

    def share(at, value):
        slot, group = stages[at]
        base = sum(len(stage[1]) + 1 for stage in stages[:at])
        sums[base + slot] = value
        for ids in group:
            pltpu.make_async_remote_copy(
                src_ref=sums.at[base + slot], dst_ref=sums.at[base + slot],
                send_sem=gsend.at[at], recv_sem=grecv.at[at],
                device_id=ids, device_id_type=MESH,
            ).start()

    def gather(at):
        size = len(stages[at][1])
        base = sum(len(stage[1]) + 1 for stage in stages[:at])
        every = sums.at[base : base + size]
        pltpu.make_async_copy(every, every, grecv.at[at]).wait()
        pltpu.make_async_copy(every, every, gsend.at[at]).wait()
        total = sums[base]
        for slot in range(1, size + 1):
            total = total + sums[base + slot]
        return total

    def fold(x):
        return jnp.sum(x[:, :128] + x[:, 128:], axis=0, keepdims=True)

    partial = jnp.concatenate([fold(c_sum), fold(v_sum)], 0)
    share(0, partial)
    face_swap((-1, 0, 0))
    face_swap((1, 0, 0))

    zlo, zhi = pack(ni - 1, zsend[0], zsend[1])
    zsend[0] = zlo
    zsend[1] = zhi
    for step in AROUND:
        if step[1] or step[2]:
            face_swap(step)

    def spread_x(i):
        return 3.0 * wx[i + 2] + 2.0 * (wx[i + 1] + wx[i + 3]) + (wx[i] + wx[i + 4])

    def spread_z(xs):
        x = jnp.concatenate(xs, 0)
        high = x.astype(BF16)
        low = (x - high.astype(F32)).astype(BF16)
        both = jnp.dot(jnp.concatenate([high, low], 0), band[...], preferred_element_type=F32)
        return both[: x.shape[0]] + both[x.shape[0] :]

    def planes_xz(group):
        done = spread_z([spread_x(i) for i in group])
        for at, i in enumerate(group):
            for h in range(2):
                wy[i, h, 8 : 8 + nj, :] = done[nj * at : nj * at + nj, 128 * h : 128 * h + 128]

    for first in range(2, ni - 2, 4):
        planes_xz(range(first, min(first + 4, ni - 2)))
    for at in range(1, len(stages)):
        share(at, gather(at - 1))
    drain(frecv.at[0], face_items(-1))

    planes_xz((0, 1, ni - 2, ni - 1))
    lines = []
    for at in range(4):
        side, t = at >> 1, at & 1
        for p in range(2):
            rows_in[at, 6 + p : 7 + p, :] = corner_in[0, side, 2 * p + t : 2 * p + t + 1, :]
            rows_in[at, 8 + ni + p : 9 + ni + p, :] = corner_in[1, side, 2 * p + t : 2 * p + t + 1, :]
        x = [rows_in[at, 6 + d : 6 + d + ni, :] for d in range(5)]
        lines.append(3.0 * x[2] + 2.0 * (x[1] + x[3]) + (x[0] + x[4]))
    done = spread_z(lines)
    for at in range(4):
        yrow[at] = done[ni * at : ni * at + ni]

    wide = iota((nj + 16, 128), 1)
    even = lax.rem(lane, 2) == 0
    rims = []
    for side in range(2):
        x = jnp.where(
            wide < 4,
            pltpu.roll(rzz[side, 0], 128 - 2 * ni, 1),
            jnp.where(wide < 2 * ni + 4, rzz[side, 1], pltpu.roll(rzz[side, 2], 2 * ni, 1)),
        )
        x = (
            3.0 * x
            + 2.0 * (pltpu.roll(x, 2, 1) + pltpu.roll(x, 126, 1))
            + (pltpu.roll(x, 4, 1) + pltpu.roll(x, 124, 1))
        )
        rzs[side] = x
        y = [rzs[side, 6 + d : 6 + d + nj, :] for d in range(5)]
        y = 3.0 * y[2] + 2.0 * (y[1] + y[3]) + (y[0] + y[4])
        y = y + jnp.where(even, 0.0, 2.0 * pltpu.roll(y, 1, 1)) if side else (
            y + jnp.where(even, 2.0 * pltpu.roll(y, 127, 1), 0.0)
        )
        rims.append(y)

    for i in range(ni):
        for h in range(2):
            half = slice(128 * h, 128 * h + 128)
            for t in range(2):
                wy[i, h, 6 + t : 7 + t, :] = yrow[t, i : i + 1, half]
                wy[i, h, 8 + nj + t : 9 + nj + t, :] = yrow[2 + t, i : i + 1, half]
            y = [wy[i, h, 6 + d : 6 + d + nj, :] for d in range(5)]
            y = 3.0 * y[2] + 2.0 * (y[1] + y[3]) + (y[0] + y[4])
            if h:
                rim = jnp.where(lane >= 126, pltpu.roll(rims[1], 122 - 2 * i, 1), 0.0)
            else:
                rim = jnp.where(lane < 2, pltpu.roll(rims[0], 124 - 2 * i, 1), 0.0)
            out[i, :, half] = y + rim
    drain(nsend.at[0], node_items(NODE_STEPS, -1))
    drain(fsend.at[0], face_items(1))
    totals[...] = gather(len(stages) - 1)


def last_pass(cells, field, totals, out, comp, vol, ends, sem):
    step = field.shape[0] // CHUNKS
    moves = [(field.at[at * step : at * step + step], out.at[at * step : at * step + step]) for at in range(CHUNKS)]
    copies = [pltpu.make_async_copy(src, dst, sem.at[at]) for at, (src, dst) in enumerate(moves)]
    for copy in copies:
        copy.start()
    ends[...] = jnp.sum(totals[...], axis=1, keepdims=True)[:, :, None] / cells
    for at, dst in enumerate((comp, vol)):
        small = pltpu.make_async_copy(ends.at[at], dst, sem.at[CHUNKS + at])
        small.start()
        copies.append(small)
    for copy in copies:
        copy.wait()


def on_device(sizes, displacement, density, stiffness):
    ni, nj, nk = density.shape
    vmem = pl.BlockSpec(memory_space=pltpu.VMEM)
    hbm = pl.BlockSpec(memory_space=pltpu.HBM)
    everyone = sizes[0] * sizes[1] * sizes[2]
    members = everyone if everyone <= FEW else sizes[0] + sizes[1] * sizes[2]
    scratch = [
        displacement.shape, density.shape, stiffness.shape,
        (3, nj, nk), (3, ni, nk), (8, nk), (2, 2, nj, 128), (3, ni, nk), (8, nk), (nj, 128),
        (2, 3, ni + 1, 2, nj + 8, 128), (2, nj // 8, ni + 1, 8, 128), (2, 6, ni, 128), (2, 6, ni, 128), (nj, nk), (ni, 128),
    ]
    later = [
        (ni + 4, nj, nk), (ni, 2, nj + 16, 128),
        (2, 2, ni, nk), (2, 2, 8, nk), (2, nj, 128), (4, ni + 16, nk), (2, 2, 8, nk),
        (2, 3, nj + 16, 128), (2, nj + 16, 128), (4, ni, nk),
        (4 * (ni + nj) * nk // 128 + 32 * nk // 128 + 6 * (nj + 16), 128), (members, 2, 128),
    ]
    field, totals = pl.pallas_call(
        functools.partial(kernel, sizes),
        out_shape=(
            jax.ShapeDtypeStruct((ni, nj, nk), F32),
            jax.ShapeDtypeStruct((2, 128), F32),
        ),
        in_specs=[hbm] * 3,
        out_specs=(vmem, vmem),
        scratch_shapes=[pltpu.VMEM(shape, F32) for shape in scratch]
        + [pltpu.VMEM((2, nj // 8, ni + 1, 48, 128), BF16), pltpu.VMEM((192, 256), BF16), pltpu.VMEM((nk, nk), BF16)]
        + [pltpu.VMEM(shape, F32) for shape in later]
        + [pltpu.SemaphoreType.DMA((count,)) for count in (5, 1, 3, 1, 1, 2, 2)]
        + [pltpu.SemaphoreType.REGULAR((1,))],
        compiler_params=pltpu.CompilerParams(
            collective_id=0, has_side_effects=True, vmem_limit_bytes=24 * 1024 * 1024
        ),
    )(*(pltpu.with_memory_space_constraint(x, pltpu.HBM) for x in (displacement, density, stiffness)))
    cells = float(ni * nj * nk * sizes[0] * sizes[1] * sizes[2])
    filtered, comp, vol = pl.pallas_call(
        functools.partial(last_pass, cells),
        out_shape=(
            jax.ShapeDtypeStruct((ni, nj, nk), F32),
            jax.ShapeDtypeStruct((1, 1), F32),
            jax.ShapeDtypeStruct((1, 1), F32),
        ),
        in_specs=[vmem] * 2,
        out_specs=(hbm, hbm, hbm),
        scratch_shapes=[pltpu.VMEM((2, 1, 1), F32), pltpu.SemaphoreType.DMA((CHUNKS + 2,))],
        compiler_params=pltpu.CompilerParams(vmem_limit_bytes=24 * 1024 * 1024),
    )(field, totals)
    return filtered, comp.reshape(()), vol.reshape(())


def solution(mesh):
    sizes = tuple(mesh.shape[axis] for axis in AXES)
    return jax.shard_map(
        functools.partial(on_device, sizes),
        mesh=mesh,
        in_specs=(P(None, "gx", "gy", "gz"), P("gx", "gy", "gz"), P()),
        out_specs=(P("gx", "gy", "gz"), P(), P()),
        check_vma=False,
    )
```

```python
import functools
import itertools
import math

import jax
import jax.numpy as jnp
from jax import lax
from jax.experimental import pallas as pl
from jax.experimental.pallas import tpu as pltpu
from jax.sharding import PartitionSpec as P

VOID = 0.001
H = (1.0, 2.0, 3.0, 2.0, 1.0)
MESH = pl.DeviceIdType.MESH
AXES = ("gx", "gy", "gz")
F32 = jnp.float32
BF16 = jnp.bfloat16
NODE_STEPS = [(a, b, c) for a in (0, 1) for b in (0, 1) for c in (0, 1) if a + b + c]
FEW = 64
CHUNKS = 4
AROUND = [(a, b, c) for a in (-1, 0, 1) for b in (-1, 0, 1) for c in (-1, 0, 1) if a or b or c]


def iota(shape, dim):
    return lax.broadcasted_iota(jnp.int32, shape, dim)


def line_sum(position, extent):
    total = None
    for d in range(5):
        at = position + (d - 2)
        term = jnp.where((at >= 0) & (at < extent), H[d], 0.0).astype(F32)
        total = term if total is None else total + term
    return total


def band_weights(stiff):
    rows, cols = 192, 128
    pick = jnp.where((iota((rows, 24), 0) >> 3) == iota((rows, 24), 1), 1.0, 0.0).astype(F32)

    def column(shape):
        col = iota(shape, 1)
        a, m, s = col >> 6, (col >> 4) & 3, col & 15
        edge = m == 3
        c = jnp.where(edge, jnp.where(s >= 3, 1, 0), s >> 3)
        m = jnp.where(edge, s - 3 * c, m)
        valid = jnp.logical_not(edge) | (s < 6)
        return 8 * m + 4 * a + c, valid, jnp.where(edge, 8, s & 7)

    total = None
    for b in (0, 1):
        q, valid, _ = column((24, cols))
        place = jnp.where((iota((24, cols), 0) == q + 2 * b) & valid, 1.0, 0.0).astype(F32)
        wide = jnp.dot(stiff, place, precision=lax.Precision.HIGHEST, preferred_element_type=F32)
        tall = jnp.dot(pick, wide, precision=lax.Precision.HIGHEST, preferred_element_type=F32)
        _, _, jj = column((rows, cols))
        term = jnp.where(jj - (iota((rows, cols), 0) & 7) == b, tall, 0.0)
        total = term if total is None else total + term
    high = total.astype(BF16)
    return jnp.concatenate([high, (total - high.astype(F32)).astype(BF16)], 1)


def kernel(
    sizes, u_hbm, rho_hbm, stiff_hbm, out, totals,
    u, rho, stiff, rx, ry, rxy, rz, ys, yd, zs,
    field, edge, line_f, line_u, inv, inv_x, parts, weights, band, wx, wy,
    ysend, corner_send, zsend, xz_send, rows_in, corner_in, rzz, xz_in, rzs, yrow, tally,
    sums, insem, nsend, nrecv, fsend, frecv, gsend, grecv, known,
):
    ni, nj, nk = rho.shape
    n = dict(zip(AXES, sizes))
    me = {axis: lax.axis_index(axis) for axis in AXES}
    ny, nz = n["gy"], n["gz"]
    down = {axis: me[axis] > 0 for axis in AXES}
    up = {axis: me[axis] < n[axis] - 1 for axis in AXES}

    loads = []
    halves = [(u_hbm.at[:, 1:, :, at : at + 128], u.at[:, 1:, :, at : at + 128]) for at in (0, 128)]
    first = [(u_hbm.at[:, 0], u.at[:, 0]), (stiff_hbm, stiff)]
    for at, (src, dst) in enumerate(first + halves + [(rho_hbm, rho)]):
        copy = pltpu.make_async_copy(src, dst, insem.at[at])
        copy.start()
        loads.append(copy)

    def hop(step):
        ids, ok = {}, None
        for axis, s in zip(AXES, step):
            if s:
                ids[axis] = me[axis] + s
                flag = up[axis] if s > 0 else down[axis]
                ok = flag if ok is None else jnp.logical_and(ok, flag)
        return ids, ok

    def minus(step):
        return tuple(-s for s in step)

    everyone = n["gx"] * ny * nz
    mine = (me["gx"] * ny + me["gy"]) * nz + me["gz"]

    def place(at):
        at = jnp.int32(at)
        return {"gx": at // (ny * nz), "gy": lax.rem(at // nz, ny), "gz": lax.rem(at, nz)}

    line = [{"gx": lax.rem(me["gx"] + off, n["gx"])} for off in range(1, n["gx"])]
    sheet = [
        {"gy": lax.rem(me["gy"] + off // nz, ny), "gz": lax.rem(me["gz"] + off % nz, nz)}
        for off in range(1, ny * nz)
    ]
    if everyone <= FEW:
        others = [at + jnp.where(at >= mine, 1, 0) for at in range(everyone - 1)]
        stages = [(mine, [place(at) for at in others])]
    else:
        stages = [(me["gx"], line), (me["gy"] * nz + me["gz"], sheet)]
    lead = mine == everyone - 1

    def hear(semaphore, amount):
        @pl.when(amount > 0)
        def _():
            pl.semaphore_wait(semaphore, amount)

    barrier = pltpu.get_barrier_semaphore()
    beyond = [n[axis] - 1 - me[axis] > 1 for axis in AXES]
    beyond = jnp.logical_or(jnp.logical_or(beyond[0], beyond[1]), beyond[2])
    lower = 0
    for step in NODE_STEPS:
        ids, ok = hop(step)
        lower = lower + jnp.where(hop(minus(step))[1], 1, 0)

        @pl.when(ok)
        def _():
            pl.semaphore_signal(barrier, inc=1, device_id=ids, device_id_type=MESH)

    @pl.when(beyond)
    def _():
        pl.semaphore_signal(barrier, inc=1, device_id=place(everyone - 1), device_id_type=MESH)


    def node_route(step):
        a, b, c = step
        if c:
            return (zs.at[0:8], rz.at[a, b, 0:8]) if b else (zs, rz.at[a, b])
        if b:
            return (yd, rxy) if a else (ys, ry)
        return u.at[:, 0], rx

    def face_route(step):
        a, b, c = step
        hi_a, hi_b, hi_c = a > 0, b > 0, c > 0
        if a and c:
            return xz_send.at[int(hi_a), int(hi_c)], xz_in.at[1 - hi_c, 1 - hi_a, 1 - b]
        if c:
            rows = (slice(nj - 8, nj), slice(0, nj), slice(0, 8))[1 - b]
            to = (slice(0, 8), slice(8, 8 + nj), slice(8 + nj, 16 + nj))[1 - b]
            return zsend.at[int(hi_c), rows], rzz.at[1 - hi_c, to]
        if a and b:
            return corner_send.at[int(hi_a), int(hi_b)], corner_in.at[1 - hi_a, 1 - hi_b]
        if b:
            at = 2 * (1 - hi_b)
            return ysend.at[int(hi_b)], rows_in.at[at : at + 2, 8 : 8 + ni]
        return (wx.at[ni : ni + 2], wx.at[0:2]) if hi_a else (wx.at[2:4], wx.at[ni + 2 : ni + 4])

    def clear(missing, *refs):
        @pl.when(jnp.logical_not(missing))
        def _():
            for ref in refs:
                ref[...] = jnp.zeros(ref.shape, F32)


    def swap(src, dst, send_sem, recv_sem, step):
        ids, sends = hop(step)

        @pl.when(sends)
        def _():
            pltpu.make_async_remote_copy(
                src_ref=src, dst_ref=dst, send_sem=send_sem, recv_sem=recv_sem,
                device_id=ids, device_id_type=MESH,
            ).start()

    def states(axis):
        if n[axis] == 1:
            return [((), True)]
        low, high = down[axis], up[axis]
        found = [((1,), jnp.logical_not(low)), ((-1,), jnp.logical_not(high))]
        return found + ([((-1, 1), jnp.logical_and(low, high))] if n[axis] > 2 else [])

    def drain(semaphore, items):
        for case in itertools.product(*(states(axis) for axis in AXES)):
            rows = sum(
                math.prod(shape) // 128
                for step, shape in items
                if all(s == 0 or s in ways for s, (ways, _) in zip(step, case))
            )
            if rows:
                flag = jnp.logical_and(jnp.logical_and(case[0][1], case[1][1]), case[2][1])

                @pl.when(flag)
                def _():
                    pltpu.make_async_copy(tally.at[0:rows], tally.at[0:rows], semaphore).wait()

    def node_items(steps, sign):
        return [(tuple(sign * s for s in step), node_route(step)[1].shape) for step in steps]

    def face_items(sign):
        return [(tuple(sign * s for s in step), face_route(step)[1].shape) for step in AROUND]

    def group_of(step):
        return 2 if step[0] else (1 if step[1] else 0)

    def node_swap(step):
        src, dst = node_route(step)
        swap(src, dst, nsend.at[0], nrecv.at[group_of(step)], minus(step))

    def arrive(which):
        drain(nrecv.at[which], node_items([s for s in NODE_STEPS if group_of(s) == which], 1))

    def face_swap(step, rows=None):
        src, dst = face_route(step)
        if rows is not None:
            src, dst = src.at[:, rows], dst.at[:, rows]
        swap(src, dst, fsend.at[0], frecv.at[0], step)

    loads[0].wait()
    hear(barrier, jnp.where(lead, everyone - 1, lower))
    node_swap((1, 0, 0))

    @pl.when(lead)
    def _():
        def greet(at, carry):
            pl.semaphore_signal(known.at[0], inc=1, device_id=place(at), device_id_type=MESH)
            return carry

        lax.fori_loop(0, everyone - 1, greet, 0)

    loads[2].wait()
    lane = iota((nj, 128), 1)
    packed = [jnp.zeros((nj, 128), F32)] * 6
    for at in range(3 * ni):
        column = u[at // ni, at % ni, :, 0:128]
        packed[at % 6] = jnp.where(lane == at, pltpu.roll(column, at, 1) if at else column, packed[at % 6])
    zs[...] = (packed[0] + packed[1]) + (packed[2] + packed[3]) + (packed[4] + packed[5])
    loads[3].wait()
    yd[...] = jnp.zeros(yd.shape, F32)
    for m in range(3):
        for i in range(ni):
            ys[m, i : i + 1, :] = u[m, i, 0:1, :]
        yd[m : m + 1, :] = u[m, 0, 0:1, :]
    for step in sorted(NODE_STEPS, key=lambda step: (sum(step), step)):
        if step != (1, 0, 0):
            node_swap(step)
    loads[1].wait()
    weights[...] = band_weights(stiff[...])
    clear(up["gx"], rx, rxy, rz.at[1], wx.at[ni + 2 : ni + 4], corner_in.at[1], xz_in.at[:, 1])
    clear(up["gy"], ry, rxy, rz.at[:, 1, 0:8], rows_in.at[2:4], corner_in.at[:, 1], rzz.at[:, 8 + nj : 16 + nj], xz_in.at[:, :, 2])
    clear(up["gz"], rz, rzz.at[1], xz_in.at[1])
    clear(down["gx"], wx.at[0:2], corner_in.at[0], xz_in.at[:, 0])
    clear(down["gy"], rows_in.at[0:2], corner_in.at[:, 0], rzz.at[:, 0:8], xz_in.at[:, :, 0])
    clear(down["gz"], rzz.at[0], xz_in.at[0])
    apart = jnp.abs(iota((nk, nk), 0) - iota((nk, nk), 1))
    band[...] = jnp.maximum(3 - apart, 0).astype(F32).astype(BF16)
    edge[...] = jnp.zeros(edge.shape, F32)

    last = iota((nj, 128), 1) == 127
    nt = nj // 8

    def sharp(x):
        return x + (x - x.astype(BF16).astype(F32))

    def layer(h, to, at, source, col):
        for m in range(3):
            x = source(m, h)
            side = source(m, 1) if h == 0 else col
            turn = 127 if h == 0 else 127 - (m * ni + at)
            moved = jnp.where(last, pltpu.roll(side, turn, 1), pltpu.roll(x, 127, 1))
            for c, y in enumerate((x, moved)):
                field[c, m, to, h, 0:nj, :] = sharp(y)
                for jt in range(nt - 1):
                    edge[h, jt, to, 3 * c + m : 3 * c + m + 1, :] = y[8 * jt + 8 : 8 * jt + 9, :]
            for jt in range(nt):
                rows = slice(8 * jt, 8 * jt + 8)
                parts[h, jt, to, 16 * m : 16 * m + 16, :] = jnp.concatenate([x[rows], moved[rows]], 0).astype(BF16)

    def own(i):
        return lambda m, h: u[m, i, :, 128 * h : 128 * h + 128]

    def next_row(c, m, to, h, x):
        field[c, m, to, h, nj : nj + 1, :] = sharp(x)
        edge[h, nt - 1, to, 3 * c + m : 3 * c + m + 1, :] = x

    def own_row(i, carry):
        at = pl.ds(i, 1)
        for h in range(2):
            for cm in range(6):
                field[cm // 3, cm % 3, i, h, nj : nj + 1, :] = line_f[h, cm, at, :]
                edge[h, nt - 1, i, cm : cm + 1, :] = line_u[h, cm, at, :]
        return carry

    none8 = jnp.zeros((8, nk), F32)

    def both(take, tiles):
        return jnp.concatenate([take(*tile) for tile in tiles], 1)

    def unit(tiles, carry):
        c_sum, v_sum = carry
        data = []
        for a in range(2):
            data.append(both(lambda i, jt, h: parts[h, jt, i + a], tiles))
            rim = both(lambda i, jt, h: edge[h, jt, i + a], tiles)
            data.append(jnp.concatenate([rim, none8], 0).astype(BF16))
        product = jnp.dot(weights[...], jnp.concatenate(data + data, 0), preferred_element_type=F32)
        energy = None
        for r in range(24):
            m, a, b, c = r >> 3, (r >> 2) & 1, (r >> 1) & 1, r & 1
            f = both(lambda i, jt, h: field[c, m, i + a, h, 8 * jt + b : 8 * jt + b + 8, :], tiles)
            term = product[8 * r : 8 * r + 8] * f
            energy = term if energy is None else energy + term

        d = both(lambda i, jt, h: rho[i, 8 * jt : 8 * jt + 8, 128 * h : 128 * h + 128], tiles)
        scale = both(
            lambda i, jt, h: inv[8 * jt : 8 * jt + 8, 128 * h : 128 * h + 128] * inv_x[pl.ds(i, 1), :], tiles
        )
        w = (-3.0 * (1.0 - VOID)) * d * d * energy * scale
        for t, (i, jt, h) in enumerate(tiles):
            wx[i + 2, 8 * jt : 8 * jt + 8, 128 * h : 128 * h + 128] = w[:, 128 * t : 128 * t + 128]
        return c_sum + (VOID + d * d * d * (1.0 - VOID)) * energy, v_sum + d

    def sweep(h):
        def body(t, carry):
            for step in (1, 2):
                layer(h, 2 * t + step, 2 * t + step, own(2 * t + step), rz[0, 0])
            for jt in range(nt - 1):
                carry = unit([(2 * t, jt, h), (2 * t + 1, jt, h)], carry)
            return carry

        return body

    def rest(h, carry):
        layer(h, ni - 1, ni - 1, own(ni - 1), rz[0, 0])
        todo = [(ni - 2, jt, h) for jt in range(nt - 1)]
        if h:
            todo += [(ni - 2, jt, 0) for jt in range((nt - 1) // 2 * 2, nt - 1)]
        for at in range(0, len(todo) // 2 * 2, 2):
            carry = unit(todo[at : at + 2], carry)
        return carry

    line_x = line_sum(me["gx"] * ni + iota((ni, 128), 0), n["gx"] * ni)
    inv_x[...] = 1.0 / line_x
    loads[4].wait()
    inv[...] = 1.0 / (
        line_sum(me["gy"] * nj + iota((nj, nk), 0), ny * nj)
        * line_sum(me["gz"] * nk + iota((nj, nk), 1), nz * nk)
    )
    carry = (none8, none8)
    layer(0, 0, 0, own(0), None)
    carry = lax.fori_loop(0, ni // 2 - 1, sweep(0), carry, unroll=7)
    carry = rest(0, carry)
    arrive(0)
    layer(1, 0, 0, own(0), rz[0, 0])
    carry = lax.fori_loop(0, ni // 2 - 1, sweep(1), carry, unroll=7)
    carry = rest(1, carry)
    ready = slice(0, nj - 8)
    face_swap((-1, 0, 0), ready)
    arrive(1)

    def row_pair(h):
        for m in range(3):
            base = ry[m]
            if h:
                mine = iota((ni, 128), 1) == iota((ni, 128), 0) + m * ni
                side = jnp.sum(jnp.where(mine, rz[0, 1, 0:1, :], 0.0), axis=1, keepdims=True)
            else:
                side = pltpu.roll(base[:, 128:256], 127, 1)
            x = base[:, 128 * h : 128 * h + 128]
            moved = jnp.where(iota((ni, 128), 1) == 127, side, pltpu.roll(x, 127, 1))
            for c, y in enumerate((x, moved)):
                line_u[h, 3 * c + m] = y
                line_f[h, 3 * c + m] = sharp(y)

    def upper(i, carry):
        return unit([(i, nt - 1, 0), (i, nt - 1, 1)], carry)

    for h in range(2):
        row_pair(h)
    lax.fori_loop(0, ni, own_row, 0, unroll=ni)
    carry = lax.fori_loop(0, ni - 1, upper, carry, unroll=ni - 1)
    zlo = zhi = jnp.zeros((nj, 128), F32)

    def pack(i, zlo, zhi):
        slot = (lane >> 1) == i + 2
        plane = wx[i + 2]
        zlo = jnp.where(slot, pltpu.roll(plane[:, 0:128], 2 * i + 4, 1), zlo)
        zhi = jnp.where(slot, pltpu.roll(plane[:, nk - 128 : nk], (2 * i + 6) % 128, 1), zhi)
        for t in range(2):
            for top, row in enumerate((t, nj - 2 + t)):
                line_at = wx[i + 2, row : row + 1, :]
                ysend[top, t, i : i + 1, :] = line_at
                if i < 2 or i >= ni - 2:
                    p = i if i < 2 else i - ni + 2
                    corner_send[int(i >= 2), top, 2 * p + t : 2 * p + t + 1, :] = line_at
        return zlo, zhi

    for i in range(ni - 1):
        zlo, zhi = pack(i, zlo, zhi)
    zsend[0] = zlo
    zsend[1] = zhi
    hear(known.at[0], jnp.where(lead, 0, 1))
    arrive(2)
    for h in range(2):
        layer(h, ni, 0, lambda m, h: rx[m, :, 128 * h : 128 * h + 128], rz[1, 0])
    for m in range(3):
        row = rxy[m : m + 1, :]
        side = pltpu.roll(rz[1, 1, 0:1, :], 127 - m * ni, 1)
        moved = jnp.where(
            iota((1, nk), 1) == nk - 1, jnp.concatenate([side, side], 1), pltpu.roll(row, nk - 1, 1)
        )
        for c, x in enumerate((row, moved)):
            for h in range(2):
                next_row(c, m, ni, h, x[:, 128 * h : 128 * h + 128])
    for jt in range(nt):
        carry = unit([(ni - 1, jt, 0), (ni - 1, jt, 1)], carry)
    c_sum, v_sum = carry

    def share(at, value):
        slot, group = stages[at]
        base = sum(len(stage[1]) + 1 for stage in stages[:at])
        sums[base + slot] = value
        for ids in group:
            pltpu.make_async_remote_copy(
                src_ref=sums.at[base + slot], dst_ref=sums.at[base + slot],
                send_sem=gsend.at[at], recv_sem=grecv.at[at],
                device_id=ids, device_id_type=MESH,
            ).start()

    def gather(at):
        size = len(stages[at][1])
        base = sum(len(stage[1]) + 1 for stage in stages[:at])
        every = sums.at[base : base + size]
        pltpu.make_async_copy(every, every, grecv.at[at]).wait()
        pltpu.make_async_copy(every, every, gsend.at[at]).wait()
        total = sums[base]
        for slot in range(1, size + 1):
            total = total + sums[base + slot]
        return total

    def fold(x):
        return jnp.sum(x[:, :128] + x[:, 128:], axis=0, keepdims=True)

    partial = jnp.concatenate([fold(c_sum), fold(v_sum)], 0)
    share(0, partial)
    face_swap((-1, 0, 0), slice(nj - 8, nj))
    face_swap((1, 0, 0))

    zlo, zhi = pack(ni - 1, zsend[0], zsend[1])
    zsend[0] = zlo
    zsend[1] = zhi
    for top in range(2):
        for side, z in enumerate((zlo, zhi)):
            tile = jnp.zeros((8, 128), F32)
            for jt in range(nt):
                turn = (4 * jt - (2 * ni if top else 4)) % 128
                z_at = z[8 * jt : 8 * jt + 8]
                tile = jnp.where(lane[0:8] >> 2 == jt, pltpu.roll(z_at, turn, 1) if turn else z_at, tile)
            xz_send[top, side] = tile
    for step in AROUND:
        if step[1] or step[2]:
            face_swap(step)

    def spread_x(i):
        return 3.0 * wx[i + 2] + 2.0 * (wx[i + 1] + wx[i + 3]) + (wx[i] + wx[i + 4])

    def spread_z(xs):
        x = jnp.concatenate(xs, 0)
        high = x.astype(BF16)
        low = (x - high.astype(F32)).astype(BF16)
        both = jnp.dot(jnp.concatenate([high, low], 0), band[...], preferred_element_type=F32)
        return both[: x.shape[0]] + both[x.shape[0] :]

    def planes_xz(group):
        done = spread_z([spread_x(i) for i in group])
        for at, i in enumerate(group):
            for h in range(2):
                wy[i, h, 8 : 8 + nj, :] = done[nj * at : nj * at + nj, 128 * h : 128 * h + 128]

    for first in range(2, ni - 2, 4):
        planes_xz(range(first, min(first + 4, ni - 2)))
    for at in range(1, len(stages)):
        share(at, gather(at - 1))
    drain(frecv.at[0], face_items(-1))

    planes_xz((0, 1, ni - 2, ni - 1))
    lines = []
    for at in range(4):
        side, t = at >> 1, at & 1
        for p in range(2):
            rows_in[at, 6 + p : 7 + p, :] = corner_in[0, side, 2 * p + t : 2 * p + t + 1, :]
            rows_in[at, 8 + ni + p : 9 + ni + p, :] = corner_in[1, side, 2 * p + t : 2 * p + t + 1, :]
        x = [rows_in[at, 6 + d : 6 + d + ni, :] for d in range(5)]
        lines.append(3.0 * x[2] + 2.0 * (x[1] + x[3]) + (x[0] + x[4]))
    done = spread_z(lines)
    for at in range(4):
        yrow[at] = done[ni * at : ni * at + ni]

    wide = iota((nj + 16, 128), 1)
    even = lax.rem(lane, 2) == 0
    rims = []
    for side in range(2):
        outer = []
        for top in range(2):
            tiles = [(0, nt - 1)] + [(1, jt) for jt in range(nt)] + [(2, 0)]
            turns = [((2 * ni + 4 if top else 0) - 4 * jt) % 128 for _, jt in tiles]
            sources = [xz_in[side, top, slot] for slot, _ in tiles]
            outer.append(
                jnp.concatenate([pltpu.roll(x, turn, 1) if turn else x for x, turn in zip(sources, turns)], 0)
            )
        inner = jnp.where(wide < 2 * ni + 4, rzz[side], 0.0)
        x = jnp.where(wide < 4, outer[0], jnp.where((wide >= 2 * ni + 4) & (wide < 2 * ni + 8), outer[1], inner))
        x = (
            3.0 * x
            + 2.0 * (pltpu.roll(x, 2, 1) + pltpu.roll(x, 126, 1))
            + (pltpu.roll(x, 4, 1) + pltpu.roll(x, 124, 1))
        )
        rzs[side] = x
        y = [rzs[side, 6 + d : 6 + d + nj, :] for d in range(5)]
        y = 3.0 * y[2] + 2.0 * (y[1] + y[3]) + (y[0] + y[4])
        y = y + jnp.where(even, 0.0, 2.0 * pltpu.roll(y, 1, 1)) if side else (
            y + jnp.where(even, 2.0 * pltpu.roll(y, 127, 1), 0.0)
        )
        rims.append(y)

    for i in range(ni):
        for h in range(2):
            half = slice(128 * h, 128 * h + 128)
            for t in range(2):
                wy[i, h, 6 + t : 7 + t, :] = yrow[t, i : i + 1, half]
                wy[i, h, 8 + nj + t : 9 + nj + t, :] = yrow[2 + t, i : i + 1, half]
            y = [wy[i, h, 6 + d : 6 + d + nj, :] for d in range(5)]
            y = 3.0 * y[2] + 2.0 * (y[1] + y[3]) + (y[0] + y[4])
            if h:
                rim = jnp.where(lane >= 126, pltpu.roll(rims[1], 122 - 2 * i, 1), 0.0)
            else:
                rim = jnp.where(lane < 2, pltpu.roll(rims[0], 124 - 2 * i, 1), 0.0)
            out[i, :, half] = y + rim
    drain(nsend.at[0], node_items(NODE_STEPS, -1))
    drain(fsend.at[0], face_items(1))
    totals[...] = gather(len(stages) - 1)


def last_pass(cells, field, totals, out, comp, vol, ends, sem):
    step = field.shape[0] // CHUNKS
    moves = [(field.at[at * step : at * step + step], out.at[at * step : at * step + step]) for at in range(CHUNKS)]
    copies = [pltpu.make_async_copy(src, dst, sem.at[at]) for at, (src, dst) in enumerate(moves)]
    for copy in copies:
        copy.start()
    ends[...] = jnp.sum(totals[...], axis=1, keepdims=True)[:, :, None] / cells
    for at, dst in enumerate((comp, vol)):
        small = pltpu.make_async_copy(ends.at[at], dst, sem.at[CHUNKS + at])
        small.start()
        copies.append(small)
    for copy in copies:
        copy.wait()


def on_device(sizes, displacement, density, stiffness):
    ni, nj, nk = density.shape
    vmem = pl.BlockSpec(memory_space=pltpu.VMEM)
    hbm = pl.BlockSpec(memory_space=pltpu.HBM)
    everyone = sizes[0] * sizes[1] * sizes[2]
    members = everyone if everyone <= FEW else sizes[0] + sizes[1] * sizes[2]
    scratch = [
        displacement.shape, density.shape, stiffness.shape,
        (3, nj, nk), (3, ni, nk), (8, nk), (2, 2, nj, 128), (3, ni, nk), (8, nk), (nj, 128),
        (2, 3, ni + 1, 2, nj + 8, 128), (2, nj // 8, ni + 1, 8, 128), (2, 6, ni, 128), (2, 6, ni, 128), (nj, nk), (ni, 128),
    ]
    later = [
        (ni + 4, nj, nk), (ni, 2, nj + 16, 128),
        (2, 2, ni, nk), (2, 2, 8, nk), (2, nj, 128), (2, 2, 8, 128), (4, ni + 16, nk), (2, 2, 8, nk),
        (2, nj + 16, 128), (2, 2, 3, 8, 128), (2, nj + 16, 128), (4, ni, nk),
        (4 * (ni + nj) * nk // 128 + 32 * nk // 128 + 6 * (nj + 16), 128), (members, 2, 128),
    ]
    field, totals = pl.pallas_call(
        functools.partial(kernel, sizes),
        out_shape=(
            jax.ShapeDtypeStruct((ni, nj, nk), F32),
            jax.ShapeDtypeStruct((2, 128), F32),
        ),
        in_specs=[hbm] * 3,
        out_specs=(vmem, vmem),
        scratch_shapes=[pltpu.VMEM(shape, F32) for shape in scratch]
        + [pltpu.VMEM((2, nj // 8, ni + 1, 48, 128), BF16), pltpu.VMEM((192, 256), BF16), pltpu.VMEM((nk, nk), BF16)]
        + [pltpu.VMEM(shape, F32) for shape in later]
        + [pltpu.SemaphoreType.DMA((count,)) for count in (5, 1, 3, 1, 1, 2, 2)]
        + [pltpu.SemaphoreType.REGULAR((1,))],
        compiler_params=pltpu.CompilerParams(
            collective_id=0, has_side_effects=True, vmem_limit_bytes=24 * 1024 * 1024
        ),
    )(*(pltpu.with_memory_space_constraint(x, pltpu.HBM) for x in (displacement, density, stiffness)))
    cells = float(ni * nj * nk * sizes[0] * sizes[1] * sizes[2])
    filtered, comp, vol = pl.pallas_call(
        functools.partial(last_pass, cells),
        out_shape=(
            jax.ShapeDtypeStruct((ni, nj, nk), F32),
            jax.ShapeDtypeStruct((1, 1), F32),
            jax.ShapeDtypeStruct((1, 1), F32),
        ),
        in_specs=[vmem] * 2,
        out_specs=(hbm, hbm, hbm),
        scratch_shapes=[pltpu.VMEM((2, 1, 1), F32), pltpu.SemaphoreType.DMA((CHUNKS + 2,))],
        compiler_params=pltpu.CompilerParams(vmem_limit_bytes=24 * 1024 * 1024),
    )(field, totals)
    return filtered, comp.reshape(()), vol.reshape(())


def solution(mesh):
    sizes = tuple(mesh.shape[axis] for axis in AXES)
    return jax.shard_map(
        functools.partial(on_device, sizes),
        mesh=mesh,
        in_specs=(P(None, "gx", "gy", "gz"), P("gx", "gy", "gz"), P()),
        out_specs=(P("gx", "gy", "gz"), P(), P()),
        check_vma=False,
    )
```
